32 devices in a mesh: il: 2 (over core), xl: 4 (over y, x), ta: 4 (over z).
Axes of the slice: x: 2, y: 2, z: 4, core: 2. Of those that a mesh axis runs over, the one named last changes fastest.
Arguments:
- traces: float32 [32, 832, 1024], P('il', 'xl', 'ta'), may hold values from -6 to 6
- bin_steps: int32 [2, 32, 832], P(None, 'il', 'xl'), may hold values from -1 to 1
Outputs:
- regridded: float32 [16, 416, 1536], P('il', 'xl', 'ta')
The draws below stay inside these ranges and needn't reach their ends.
Inputs may be any that keep to these rules, and one draw needn't show every extreme that they name: `bin_steps`: every entry is -1, 0 or 1.
All inputs are finite; a program needn't handle non-finite values.
Results may differ from the reference program's by a relative error of at most 0.0001.
Values sent between devices are 32-bit elements; how exact they have to be, the bound alone decides.
A program may use at most 128 MiB of HBM per device.

```python
import jax
import jax.numpy as jnp
from jax import lax

CT = 256
TAPS = 16
P_SIZE = 3
Q = 2
NI = 32
NX = 832
NT = 1024
BI = 16
BX = 416
N_TA = 4


def set_ends(entries, own_key, low, largest):
    longest = entries.shape.index(max(entries.shape))
    spots = []
    for shift in (0, 1):
        where = [jax.random.randint(jax.random.fold_in(own_key, axis), (), 0, length) for axis, length in enumerate(entries.shape)]
        where[longest] = (where[longest] + shift) % entries.shape[longest]
        spots.append(tuple(where))
    return entries.at[spots[0]].set(low).at[spots[1]].set(largest)


def block_scale(key, shape, cuts, smallest, high):
    loudness, own = 1.0, jax.random.fold_in(key, 6)
    for dim, blocks in cuts:
        draws = jnp.exp(jax.random.uniform(jax.random.fold_in(own, dim), (blocks,), jnp.float32, smallest / len(cuts), high / len(cuts)))
        loudness = loudness * jnp.repeat(draws, shape[dim] // blocks).reshape([-1 if axis == dim else 1 for axis in range(len(shape))])
    return loudness


def gaussian(key, dims, spread, most, split=(), kind=jnp.bfloat16):
    drawn = spread * jax.random.normal(key, dims, jnp.float32)
    if split:
        drawn = drawn * block_scale(key, dims, split, -0.22, 0.18)
    return jnp.clip(drawn, -most, most).astype(kind)


def setup_inputs(seed: int = 0) -> dict:
    streams_of = jax.random.split(jax.random.key(seed), 3)
    traces = gaussian(streams_of[0], (NI, NX, NT), 1.0, 6.0, ((0, 2), (1, 4), (2, 4)), jnp.float32)
    bin_steps = set_ends(jax.random.randint(streams_of[1], (2, NI, NX), -1, 2), jax.random.fold_in(streams_of[1], 1), -1, 1).astype(jnp.int32)
    return {"traces": traces, "bin_steps": bin_steps}


def lanczos_table(row_count, col_count, tap_reach, ratio_p, ratio_q):
    row_ids = lax.broadcasted_iota(jnp.int32, (row_count, col_count), 0)
    col_ids = lax.broadcasted_iota(jnp.int32, (row_count, col_count), 1)
    offset = (col_ids * ratio_q - (row_ids - tap_reach) * ratio_p).astype(jnp.float32) / jnp.float32(ratio_p)
    inside = jnp.abs(offset) < jnp.float32(tap_reach)
    weights = jnp.sinc(offset) * jnp.sinc(offset / jnp.float32(tap_reach))
    return jnp.where(inside, weights, jnp.zeros_like(weights))


def reference(traces, bin_steps):
    tap_reach = TAPS // 2
    bin_total = jnp.zeros((BI + 2, BX + 2, NT), jnp.float32)
    fold_count = jnp.zeros((BI + 2, BX + 2), jnp.float32)
    for row_phase in (0, 1):
        for col_phase in (0, 1):
            sub_traces = traces[row_phase::2, col_phase::2]
            step_il = bin_steps[0, row_phase::2, col_phase::2]
            step_xl = bin_steps[1, row_phase::2, col_phase::2]
            for shift_il in (-1, 0, 1):
                for shift_xl in (-1, 0, 1):
                    chosen = ((step_il == shift_il) & (step_xl == shift_xl)).astype(jnp.float32)
                    widths = ((1 + shift_il, 1 - shift_il), (1 + shift_xl, 1 - shift_xl))
                    bin_total = bin_total + jnp.pad(sub_traces * chosen[:, :, None], widths + ((0, 0),))
                    fold_count = fold_count + jnp.pad(chosen, widths)
    stacked = bin_total[1:-1, 1:-1] / jnp.maximum(fold_count[1:-1, 1:-1], 1.0)[:, :, None]
    padded = jnp.pad(stacked, ((0, 0), (0, 0), (tap_reach, tap_reach)))
    taps_table = lanczos_table(CT + 2 * tap_reach, CT * P_SIZE // Q, tap_reach, P_SIZE, Q)
    blocks = []
    for block_idx in range(N_TA):
        block_rows = padded[:, :, block_idx * CT: block_idx * CT + CT + 2 * tap_reach].reshape(BI * BX, CT + 2 * tap_reach)
        result = jnp.dot(block_rows, taps_table, precision=lax.Precision.HIGHEST, preferred_element_type=jnp.float32)
        blocks.append(result.reshape(BI, BX, CT * P_SIZE // Q))
    return jnp.concatenate(blocks, axis=2)
```

```python
import functools

import numpy as np
import jax
import jax.numpy as jnp
from jax import lax
from jax.experimental import pallas as pl
from jax.experimental.pallas import tpu as pltpu
from jax.sharding import PartitionSpec as P

TAPS = 16
P_SIZE = 3
Q = 2
MESH = pl.DeviceIdType.MESH
F32, BF16 = jnp.float32, jnp.bfloat16


def lanczos_table(span):
    reach = TAPS // 2
    rows = np.arange(span + 2 * reach)[:, None] - reach
    cols = np.arange(span * P_SIZE // Q)[None, :]
    offset = (cols * Q - rows * P_SIZE).astype(np.float64) / P_SIZE
    weights = np.sinc(offset) * np.sinc(offset / reach)
    return np.where(np.abs(offset) < reach, weights, 0.0).astype(np.float32)


def split_table(table):
    high = table.astype(BF16)
    low = (table - high.astype(np.float32)).astype(BF16)
    return high, low


def halves(values):
    high = values.astype(BF16)
    low = (values - high.astype(F32)).astype(BF16)
    return high, low


def dot(a, b):
    return jnp.dot(a, b, preferred_element_type=F32)


def kernel(n_xl, n_ta, traces, steps, t_high, t_low, t_edge, out, x, acc, rim_send, rim_recv,
           il_recv, corner_recv, halo_send, halo_recv, load_sem, send_sem, recv_sem):
    n_rows, n_cols, span = x.shape
    n_pairs = n_rows // 2
    own_cols = n_cols // 2
    reach = TAPS // 2
    il, xl, ta = lax.axis_index("il"), lax.axis_index("xl"), lax.axis_index("ta")
    other = 1 - il
    xl_up, xl_down = lax.rem(xl + 1, n_xl), lax.rem(xl + n_xl - 1, n_xl)
    ta_up, ta_down = lax.rem(ta + 1, n_ta), lax.rem(ta + n_ta - 1, n_ta)

    loads = []
    for p in range(n_pairs):
        load = pltpu.make_async_copy(traces.at[pl.ds(2 * p, 2)], x.at[pl.ds(2 * p, 2)], load_sem.at[p])
        load.start()
        loads.append(load)
    barrier = pltpu.get_barrier_semaphore()
    partners = ({"il": other}, {"xl": xl_up}, {"xl": xl_down}, {"il": other, "xl": xl_up},
                {"il": other, "xl": xl_down}, {"ta": ta_up}, {"ta": ta_down})
    for partner in partners:
        pl.semaphore_signal(barrier, inc=1, device_id=partner, device_id_type=MESH)

    split = own_cols // 16 * 16
    if split == n_cols or split < 16:
        raise ValueError("column count")
    ranges = []
    for start, stop in ((0, split), (split, n_cols)):
        first = start // 2 // 8 * 8
        last = (stop - 1) // 2 + 2
        ranges.append((start, stop, first, (last + 1 - first + 7) // 8 * 8))
    col = lax.broadcasted_iota(jnp.int32, (n_rows, n_cols), 1)
    bin_col = lax.shift_right_logical(col, 1) + steps[1] + 1
    bin_row = steps[0] + 1
    acc[...] = jnp.zeros_like(acc)
    codes = [bin_row * height + bin_col - first for _, _, first, height in ranges]
    for p in range(n_pairs):
        loads[p].wait()
        for (start, stop, first, height), code in zip(ranges, codes):
            depth = 2 * (stop - start)
            key = jnp.concatenate([code[2 * p: 2 * p + 1, start:stop], code[2 * p + 1: 2 * p + 2, start:stop]], axis=1)
            rows = lax.broadcasted_iota(jnp.int32, (3 * height, depth), 0)
            chosen = jnp.where(rows == key, 1.0, 0.0).astype(BF16)
            values = jnp.concatenate([x[2 * p, start:stop, :], x[2 * p + 1, start:stop, :]], axis=0)
            high, low = halves(values)
            sums = dot(chosen, high) + dot(chosen, low)
            folds = dot(chosen, jnp.ones((depth, 128), BF16))
            for r in range(3):
                acc[p + r, first: first + height, :span] += sums[r * height: (r + 1) * height]
                acc[p + r, first: first + height, span:] += folds[r * height: (r + 1) * height]

    rim_row = jnp.where(il == 0, n_pairs + 1, 0)
    own_row = jnp.where(il == 0, n_pairs, 1)
    pl.semaphore_wait(barrier, len(partners))

    def send(src, dst, slot, partner):
        copy = pltpu.make_async_remote_copy(src_ref=src, dst_ref=dst, send_sem=send_sem.at[slot],
                                            recv_sem=recv_sem.at[slot], device_id=partner, device_id_type=MESH)
        copy.start()
        return copy

    copies = [send(acc.at[rim_row], il_recv, 0, {"il": other})]
    for r in range(n_pairs + 2):
        rim_send[0, r] = acc[r, own_cols + 1: own_cols + 2, :]
        rim_send[1, r] = acc[r, 0:1, :]
    for d, where in ((0, xl_up), (1, xl_down)):
        copies.append(send(rim_send.at[d], rim_recv.at[d], 1 + d, {"xl": where}))
        copies.append(send(rim_send.at[d, rim_row], corner_recv.at[d], 3 + d, {"il": other, "xl": where}))
    for copy in copies:
        copy.wait()
    acc[own_row] = acc[own_row] + il_recv[...]
    for d, (column, real) in enumerate(((1, xl > 0), (own_cols, xl < n_xl - 1))):
        for r in range(1, n_pairs + 1):
            acc[r, column: column + 1, :] += jnp.where(real, rim_recv[d, r], 0.0)
        acc[own_row, column: column + 1, :] += jnp.where(real, corner_recv[d], 0.0)

    for b in range(n_pairs):
        lanes = slice(b * 128, b * 128 + own_cols)
        halo_send[0, :, lanes] = acc[b + 1, 1: own_cols + 1, :128].T[:reach]
        halo_send[1, :, lanes] = acc[b + 1, 1: own_cols + 1, span - 128: span].T[128 - reach:]
    halos = [send(halo_send.at[1], halo_recv.at[0], 5, {"ta": ta_up}),
             send(halo_send.at[0], halo_recv.at[1], 6, {"ta": ta_down})]
    for b in range(n_pairs):
        high, low = halves(acc[b + 1, 1: own_cols + 1, :span])
        out[b] = dot(high, t_high[...]) + (dot(low, t_high[...]) + dot(high, t_low[...]))
    for copy in halos:
        copy.wait()
    for b in range(n_pairs):
        lanes = slice(b * 128, (b + 1) * 128)
        before = jnp.where(ta > 0, halo_recv[0, :, lanes], 0.0)
        after = jnp.where(ta < n_ta - 1, halo_recv[1, :, lanes], 0.0)
        edges = jnp.concatenate([before, after], axis=0).T[:own_cols]
        high, low = halves(edges)
        edge_high, edge_low = t_edge[0], t_edge[1]
        edge = dot(high, edge_high) + (dot(low, edge_high) + dot(high, edge_low))
        scale = 1.0 / jnp.maximum(acc[b + 1, 1: own_cols + 1, span:], 1.0)
        out[b] = (out[b] + edge) * jnp.concatenate([scale] * (edge.shape[1] // 128), axis=1)


def shards(n_xl, n_ta, traces, bin_steps):
    n_rows, n_cols, span = traces.shape
    n_pairs, own_cols = n_rows // 2, n_cols // 2
    reach = TAPS // 2
    padded = (own_cols + 2 + 7) // 8 * 8
    width = span + 128
    out_span = span * P_SIZE // Q
    table = lanczos_table(span)
    t_high, t_low = split_table(table[reach:-reach])
    t_edge = np.stack(split_table(np.concatenate([table[:reach], table[-reach:]])))
    vmem = pl.BlockSpec(memory_space=pltpu.VMEM)
    return pl.pallas_call(
        functools.partial(kernel, n_xl, n_ta),
        out_shape=jax.ShapeDtypeStruct((n_pairs, own_cols, out_span), F32),
        in_specs=[pl.BlockSpec(memory_space=pl.ANY)] + [vmem] * 4,
        out_specs=vmem,
        scratch_shapes=[
            pltpu.VMEM((n_rows, n_cols, span), F32),
            pltpu.VMEM((n_pairs + 2, padded, width), F32),
            pltpu.VMEM((2, n_pairs + 2, 1, width), F32),
            pltpu.VMEM((2, n_pairs + 2, 1, width), F32),
            pltpu.VMEM((padded, width), F32),
            pltpu.VMEM((2, 1, width), F32),
            pltpu.VMEM((2, reach, n_pairs * 128), F32),
            pltpu.VMEM((2, reach, n_pairs * 128), F32),
            pltpu.SemaphoreType.DMA((n_pairs,)),
            pltpu.SemaphoreType.DMA((7,)),
            pltpu.SemaphoreType.DMA((7,)),
        ],
        compiler_params=pltpu.CompilerParams(collective_id=0, has_side_effects=True),
    )(traces, bin_steps, jnp.asarray(t_high), jnp.asarray(t_low), jnp.asarray(t_edge))


def solution(mesh):
    if mesh.shape["il"] != 2:
        raise ValueError("il size")
    return jax.shard_map(
        functools.partial(shards, mesh.shape["xl"], mesh.shape["ta"]),
        mesh=mesh,
        in_specs=(P("il", "xl", "ta"), P(None, "il", "xl")),
        out_specs=P("il", "xl", "ta"),
        check_vma=False,
    )
```

```python
import functools

import numpy as np
import jax
import jax.numpy as jnp
from jax import lax
from jax.experimental import pallas as pl
from jax.experimental.pallas import tpu as pltpu
from jax.sharding import PartitionSpec as P

TAPS = 16
P_SIZE = 3
Q = 2
MESH = pl.DeviceIdType.MESH
F32, BF16 = jnp.float32, jnp.bfloat16


def lanczos_table(span):
    reach = TAPS // 2
    rows = np.arange(span + 2 * reach)[:, None] - reach
    cols = np.arange(span * P_SIZE // Q)[None, :]
    offset = (cols * Q - rows * P_SIZE).astype(np.float64) / P_SIZE
    weights = np.sinc(offset) * np.sinc(offset / reach)
    return np.where(np.abs(offset) < reach, weights, 0.0).astype(np.float32)


def split_table(table):
    high = table.astype(BF16)
    low = (table - high.astype(np.float32)).astype(BF16)
    return high, low


def halves(values):
    high = values.astype(BF16)
    low = (values - high.astype(F32)).astype(BF16)
    return high, low


def dot(a, b):
    return jnp.dot(a, b, preferred_element_type=F32)


def column_ranges(n_cols):
    split = n_cols // 2 // 16 * 16
    if split < 16 or n_cols % 16:
        raise ValueError("column count")
    ranges = []
    for start, stop in ((0, split), (split, n_cols)):
        first = start // 2 // 8 * 8
        last = (stop - 1) // 2 + 2
        ranges.append((start, stop, first, (last + 1 - first + 7) // 8 * 8))
    return ranges


def binning(n_xl, n_ta, traces, steps_hbm, t_high_hbm, t_low_hbm, main, scale, halo_out, x, edge_x, steps, t_high, t_low, keys,
            acc, rim_send, rim_recv, il_recv, corner_recv, halo_send, halo_recv, load_sem, edge_sem, table_sem,
            send_sem, recv_sem):
    n_rows, n_cols, span = x.shape
    n_pairs = n_rows // 2
    own_cols = n_cols // 2
    reach = TAPS // 2
    il, xl, ta = lax.axis_index("il"), lax.axis_index("xl"), lax.axis_index("ta")
    other = 1 - il
    has_xl = (xl < n_xl - 1, xl > 0)
    has_ta = (ta < n_ta - 1, ta > 0)
    xl_at, ta_at = (xl + 1, xl - 1), (ta + 1, ta - 1)

    def when(condition, work):
        pl.when(condition)(work)

    def pair(p):
        return jnp.where(il == 0, n_pairs - 1 - p, p)

    step_load = pltpu.make_async_copy(steps_hbm, steps, table_sem.at[2])
    step_load.start()
    edge_loads = [pltpu.make_async_copy(traces.at[:, pl.ds(start, 8)], edge_x.at[d], edge_sem.at[d])
                  for d, start in enumerate((n_cols - 8, 0))]
    for load in edge_loads:
        load.start()
    loads = []
    for p in range(n_pairs):
        rows = pl.ds(2 * pair(p), 2)
        loads.append(pltpu.make_async_copy(traces.at[rows], x.at[rows], load_sem.at[p]))
    for load in loads:
        load.start()
    table_loads = [pltpu.make_async_copy(t_high_hbm, t_high, table_sem.at[0]),
                   pltpu.make_async_copy(t_low_hbm, t_low, table_sem.at[1])]
    for load in table_loads:
        load.start()

    barrier = pltpu.get_barrier_semaphore()

    def greet(partner):
        pl.semaphore_signal(barrier, inc=1, device_id=partner, device_id_type=MESH)

    greet({"il": other})
    for d in range(2):
        def both(d=d):
            greet({"xl": xl_at[d]})
            greet({"il": other, "xl": xl_at[d]})
        when(has_xl[d], both)
        when(has_ta[d], lambda d=d: greet({"ta": ta_at[d]}))

    acc[...] = jnp.zeros_like(acc)
    step_load.wait()
    ranges = column_ranges(n_cols)
    col = lax.broadcasted_iota(jnp.int32, (n_rows, n_cols), 1)
    bin_col = lax.shift_right_logical(col, 1) + steps[1] + 1
    bin_row = steps[0] + 1
    for k, (start, stop, first, height) in enumerate(ranges):
        code = bin_row * height + bin_col - first
        for p in range(n_pairs):
            keys[k, p, :, :2 * (stop - start)] = jnp.concatenate(
                [code[2 * p: 2 * p + 1, start:stop], code[2 * p + 1: 2 * p + 2, start:stop]], axis=1)

    def one_hot(key, height):
        rows = lax.broadcasted_iota(jnp.int32, (height, key.shape[1]), 0)
        return jnp.where(rows == key, 1.0, 0.0).astype(BF16)

    def totals(chosen, values):
        high, low = halves(values)
        return (dot(chosen, high) + dot(chosen, low), dot(chosen, jnp.ones((values.shape[0], 128), BF16)))

    def bin_pair(p):
        at = pair(p)
        loads[p].wait()
        for k, (start, stop, first, height) in enumerate(ranges):
            key = keys[k, at][:, :2 * (stop - start)]
            values = jnp.concatenate([x[2 * at, start:stop, :], x[2 * at + 1, start:stop, :]], axis=0)
            sums, folds = totals(one_hot(key, 3 * height), values)
            for r in range(3):
                acc[at + r, first: first + height, :span] += sums[r * height: (r + 1) * height]
                acc[at + r, first: first + height, span:] += folds[r * height: (r + 1) * height]

    def remote(src, dst, slot, partner):
        return pltpu.make_async_remote_copy(src_ref=src, dst_ref=dst, send_sem=send_sem.at[slot],
                                            recv_sem=recv_sem.at[slot], device_id=partner, device_id_type=MESH)

    rim_row = jnp.where(il == 0, n_pairs + 1, 0)
    own_row = jnp.where(il == 0, n_pairs, 1)
    to_other = remote(acc.at[rim_row], il_recv, 0, {"il": other})
    rims = [(remote(rim_send.at[d], rim_recv.at[d], 1 + d, {"xl": xl_at[d]}),
             remote(rim_send.at[d, rim_row], corner_recv.at[d], 3 + d, {"il": other, "xl": xl_at[d]}))
            for d in range(2)]

    row = lax.broadcasted_iota(jnp.int32, (n_rows, n_cols), 0)
    rim_bin = bin_row + lax.shift_right_logical(row, 1)
    for load in edge_loads:
        load.wait()
    for d, (start, column) in enumerate(((n_cols - 8, own_cols + 1), (0, 0))):
        target = jnp.where(bin_col == column, rim_bin, -1)
        key = jnp.concatenate([target[i: i + 1, start: start + 8] for i in range(n_rows)], axis=1)
        sums, folds = totals(one_hot(key, (n_pairs + 2 + 7) // 8 * 8), edge_x[d].reshape(n_rows * 8, span))
        for r in range(n_pairs + 2):
            rim_send[d, r, :, :span] = sums[r: r + 1]
            rim_send[d, r, :, span:] = folds[r: r + 1]
    bin_pair(0)
    peers = 1
    for d in range(2):
        peers = peers + jnp.where(has_xl[d], 2, 0) + jnp.where(has_ta[d], 1, 0)
    pl.semaphore_wait(barrier, peers)
    to_other.start()
    for d in range(2):
        def go(d=d):
            for copy in rims[d]:
                copy.start()
        when(has_xl[d], go)
    for p in range(1, n_pairs):
        bin_pair(p)
    to_other.wait_recv()
    acc[own_row] = acc[own_row] + il_recv[...]
    for d, column in enumerate((1, own_cols)):
        def add(d=d, column=column):
            for copy in rims[d]:
                copy.wait_recv()
            for r in range(1, n_pairs + 1):
                acc[r, column: column + 1, :] += rim_recv[d, r]
            acc[own_row, column: column + 1, :] += corner_recv[d]
        when(has_xl[1 - d], add)

    halos = [remote(halo_send.at[d], halo_recv.at[d], 5 + d, {"ta": ta_at[d]}) for d in range(2)]
    for b in range(n_pairs):
        lanes = slice(b * 128, b * 128 + own_cols)
        halo_send[0, :, lanes] = acc[b + 1, 1: own_cols + 1, span - 128: span].T[128 - reach:]
        halo_send[1, :, lanes] = acc[b + 1, 1: own_cols + 1, :128].T[:reach]
    for d in range(2):
        when(has_ta[d], halos[d].start)
    for load in table_loads:
        load.wait()
    for b in range(n_pairs):
        high, low = halves(acc[b + 1, 1: own_cols + 1, :span])
        main[b] = dot(high, t_high[...]) + (dot(low, t_high[...]) + dot(high, t_low[...]))
        scale[b] = 1.0 / jnp.maximum(acc[b + 1, 1: own_cols + 1, span:], 1.0)
    for d in range(2):
        def arrived(d=d):
            halos[d].wait_recv()
            halo_out[d] = halo_recv[d]

        def absent(d=d):
            halo_out[d] = jnp.zeros_like(halo_recv[d])
        when(has_ta[1 - d], arrived)
        when(jnp.logical_not(has_ta[1 - d]), absent)
    for d in range(2):
        when(has_ta[d], halos[d].wait_send)
        def sent(d=d):
            for copy in rims[d]:
                copy.wait_send()
        when(has_xl[d], sent)
    to_other.wait_send()


def finish(main, scale, halo, t_edge, out, staged, out_sem):
    n_pairs, own_cols, width = main.shape
    writes = []
    for b in range(n_pairs):
        lanes = slice(b * 128, (b + 1) * 128)
        edges = jnp.concatenate([halo[0, :, lanes], halo[1, :, lanes]], axis=0).T[:own_cols]
        high, low = halves(edges)
        edge = dot(high, t_edge[0]) + (dot(low, t_edge[0]) + dot(high, t_edge[1]))
        staged[b] = (main[b] + edge) * jnp.concatenate([scale[b]] * (width // 128), axis=1)
        write = pltpu.make_async_copy(staged.at[b], out.at[b], out_sem.at[b])
        write.start()
        writes.append(write)
    for write in writes:
        write.wait()


def shards(n_xl, n_ta, traces, bin_steps):
    n_rows, n_cols, span = traces.shape
    n_pairs, own_cols = n_rows // 2, n_cols // 2
    reach = TAPS // 2
    padded = (own_cols + 2 + 7) // 8 * 8
    width = span + 128
    out_span = span * P_SIZE // Q
    table = lanczos_table(span)
    t_high, t_low = split_table(table[reach:-reach])
    t_edge = np.stack(split_table(np.concatenate([table[:reach], table[-reach:]])))
    vmem = pl.BlockSpec(memory_space=pltpu.VMEM)
    hbm = pl.BlockSpec(memory_space=pltpu.HBM)
    main, scale, halo = pl.pallas_call(
        functools.partial(binning, n_xl, n_ta),
        out_shape=(pltpu.VMEM((n_pairs, own_cols, out_span), F32), pltpu.VMEM((n_pairs, own_cols, 128), F32),
                   pltpu.VMEM((2, reach, n_pairs * 128), F32)),
        in_specs=[hbm] * 4,
        out_specs=[vmem] * 3,
        scratch_shapes=[
            pltpu.VMEM((n_rows, n_cols, span), F32),
            pltpu.VMEM((2, n_rows, 8, span), F32),
            pltpu.VMEM((2, n_rows, n_cols), jnp.int32),
            pltpu.VMEM(t_high.shape, BF16),
            pltpu.VMEM(t_low.shape, BF16),
            pltpu.VMEM((2, n_pairs, 1, (n_cols + 32 + 127) // 128 * 128), jnp.int32),
            pltpu.VMEM((n_pairs + 2, padded, width), F32),
            pltpu.VMEM((2, n_pairs + 2, 1, width), F32),
            pltpu.VMEM((2, n_pairs + 2, 1, width), F32),
            pltpu.VMEM((padded, width), F32),
            pltpu.VMEM((2, 1, width), F32),
            pltpu.VMEM((2, reach, n_pairs * 128), F32),
            pltpu.VMEM((2, reach, n_pairs * 128), F32),
            pltpu.SemaphoreType.DMA((n_pairs,)),
            pltpu.SemaphoreType.DMA((2,)),
            pltpu.SemaphoreType.DMA((3,)),
            pltpu.SemaphoreType.DMA((7,)),
            pltpu.SemaphoreType.DMA((7,)),
        ],
        compiler_params=pltpu.CompilerParams(collective_id=0, has_side_effects=True, vmem_limit_bytes=24 * 2**20),
        name="binning",
    )(*[pltpu.with_memory_space_constraint(a, pltpu.HBM) for a in (traces, bin_steps, jnp.asarray(t_high), jnp.asarray(t_low))])
    return pl.pallas_call(
        finish,
        out_shape=jax.ShapeDtypeStruct((n_pairs, own_cols, out_span), F32),
        in_specs=[vmem] * 4,
        out_specs=hbm,
        scratch_shapes=[pltpu.VMEM((n_pairs, own_cols, out_span), F32), pltpu.SemaphoreType.DMA((n_pairs,))],
        compiler_params=pltpu.CompilerParams(vmem_limit_bytes=16 * 2**20),
        name="finish",
    )(main, scale, halo, jnp.asarray(t_edge))


def solution(mesh):
    if mesh.shape["il"] != 2:
        raise ValueError("il size")
    return jax.shard_map(
        functools.partial(shards, mesh.shape["xl"], mesh.shape["ta"]),
        mesh=mesh,
        in_specs=(P("il", "xl", "ta"), P(None, "il", "xl")),
        out_specs=P("il", "xl", "ta"),
        check_vma=False,
    )
```

```python
import functools

import numpy as np
import jax
import jax.numpy as jnp
from jax import lax
from jax.experimental import pallas as pl
from jax.experimental.pallas import tpu as pltpu
from jax.sharding import PartitionSpec as P

TAPS = 16
P_SIZE = 3
Q = 2
MESH = pl.DeviceIdType.MESH
F32, BF16 = jnp.float32, jnp.bfloat16


def lanczos_table(span):
    reach = TAPS // 2
    rows = np.arange(span + 2 * reach)[:, None] - reach
    cols = np.arange(span * P_SIZE // Q)[None, :]
    offset = (cols * Q - rows * P_SIZE).astype(np.float64) / P_SIZE
    weights = np.sinc(offset) * np.sinc(offset / reach)
    return np.where(np.abs(offset) < reach, weights, 0.0).astype(np.float32)


def split_table(table):
    high = table.astype(BF16)
    low = (table - high.astype(np.float32)).astype(BF16)
    return high, low


def halves(values):
    high = values.astype(BF16)
    low = (values - high.astype(F32)).astype(BF16)
    return high, low


def dot(a, b):
    return jnp.dot(a, b, preferred_element_type=F32)


def column_ranges(n_cols):
    split = n_cols // 2 // 16 * 16
    if split < 16 or n_cols % 16:
        raise ValueError("column count")
    ranges = []
    for start, stop in ((0, split), (split, n_cols)):
        first = start // 2 // 8 * 8
        last = (stop - 1) // 2 + 2
        ranges.append((start, stop, first, (last + 1 - first + 7) // 8 * 8))
    return ranges


def binning(n_xl, n_ta, traces, steps_hbm, t_high_hbm, t_low_hbm, main, halo_out, x, edge_x, steps, t_high, t_low, keys,
            acc, stacked, rim_send, rim_recv, il_recv, corner_recv, halo_send, halo_recv, load_sem, edge_sem, table_sem,
            send_sem, recv_sem):
    n_rows, n_cols, span = x.shape
    n_pairs = n_rows // 2
    own_cols = n_cols // 2
    reach = TAPS // 2
    il, xl, ta = lax.axis_index("il"), lax.axis_index("xl"), lax.axis_index("ta")
    other = 1 - il
    has_xl = (xl < n_xl - 1, xl > 0)
    has_ta = (ta < n_ta - 1, ta > 0)
    xl_at, ta_at = (xl + 1, xl - 1), (ta + 1, ta - 1)

    def when(condition, work):
        pl.when(condition)(work)

    def pair(p):
        return jnp.where(il == 0, n_pairs - 1 - p, p)

    step_load = pltpu.make_async_copy(steps_hbm, steps, table_sem.at[2])
    step_load.start()
    edge_loads = [pltpu.make_async_copy(traces.at[:, pl.ds(start, 8)], edge_x.at[d], edge_sem.at[d])
                  for d, start in enumerate((n_cols - 8, 0))]
    for load in edge_loads:
        load.start()
    loads = []
    for p in range(n_pairs):
        rows = pl.ds(2 * pair(p), 2)
        loads.append(pltpu.make_async_copy(traces.at[rows], x.at[rows], load_sem.at[p]))

    def load_pair(p):
        rows = pl.ds(2 * pair(p), 2)
        pltpu.make_async_copy(traces.at[rows], x.at[rows], load_sem.at[p]).start()

    pl.loop(0, n_pairs)(load_pair)
    table_loads = [pltpu.make_async_copy(t_high_hbm, t_high, table_sem.at[0]),
                   pltpu.make_async_copy(t_low_hbm, t_low, table_sem.at[1])]
    for load in table_loads:
        load.start()

    barrier = pltpu.get_barrier_semaphore()

    def greet(partner):
        pl.semaphore_signal(barrier, inc=1, device_id=partner, device_id_type=MESH)

    greet({"il": other})
    for d in range(2):
        def both(d=d):
            greet({"xl": xl_at[d]})
            greet({"il": other, "xl": xl_at[d]})
        when(has_xl[d], both)
        when(has_ta[d], lambda d=d: greet({"ta": ta_at[d]}))

    acc[...] = jnp.zeros_like(acc)
    step_load.wait()
    ranges = column_ranges(n_cols)
    col = lax.broadcasted_iota(jnp.int32, (n_rows, n_cols), 1)
    bin_col = lax.shift_right_logical(col, 1) + steps[1] + 1
    bin_row = steps[0] + 1
    for k, (start, stop, first, height) in enumerate(ranges):
        code = bin_row * height + bin_col - first
        for p in range(n_pairs):
            keys[k, p, :, :2 * (stop - start)] = jnp.concatenate(
                [code[2 * p: 2 * p + 1, start:stop], code[2 * p + 1: 2 * p + 2, start:stop]], axis=1)

    def one_hot(key, height):
        rows = lax.broadcasted_iota(jnp.int32, (height, key.shape[1]), 0)
        return jnp.where(rows == key, 1.0, 0.0).astype(BF16)

    def totals(chosen, values):
        high, low = halves(values)
        return (dot(chosen, high) + dot(chosen, low), dot(chosen, jnp.ones((values.shape[0], 128), BF16)))

    def bin_pair(p):
        at = pair(p)
        loads[p].wait()
        for k, (start, stop, first, height) in enumerate(ranges):
            key = keys[k, at][:, :2 * (stop - start)]
            values = jnp.concatenate([x[2 * at, start:stop, :], x[2 * at + 1, start:stop, :]], axis=0)
            sums, folds = totals(one_hot(key, 3 * height), values)
            for r in range(3):
                acc[at + r, first: first + height, :span] += sums[r * height: (r + 1) * height]
                acc[at + r, first: first + height, span:] += folds[r * height: (r + 1) * height]

    def remote(src, dst, slot, partner):
        return pltpu.make_async_remote_copy(src_ref=src, dst_ref=dst, send_sem=send_sem.at[slot],
                                            recv_sem=recv_sem.at[slot], device_id=partner, device_id_type=MESH)

    rim_row = jnp.where(il == 0, n_pairs + 1, 0)
    own_row = jnp.where(il == 0, n_pairs, 1)
    to_other = remote(acc.at[rim_row], il_recv, 0, {"il": other})
    rims = [(remote(rim_send.at[d], rim_recv.at[d], 1 + d, {"xl": xl_at[d]}),
             remote(rim_send.at[d, rim_row], corner_recv.at[d], 3 + d, {"il": other, "xl": xl_at[d]}))
            for d in range(2)]

    row = lax.broadcasted_iota(jnp.int32, (n_rows, n_cols), 0)
    rim_bin = bin_row + lax.shift_right_logical(row, 1)
    for load in edge_loads:
        load.wait()
    for d, (start, column) in enumerate(((n_cols - 8, own_cols + 1), (0, 0))):
        target = jnp.where(bin_col == column, rim_bin, -1)
        key = jnp.concatenate([target[i: i + 1, start: start + 8] for i in range(n_rows)], axis=1)
        sums, folds = totals(one_hot(key, (n_pairs + 2 + 7) // 8 * 8), edge_x[d].reshape(n_rows * 8, span))
        for r in range(n_pairs + 2):
            rim_send[d, r, :, :span] = sums[r: r + 1]
            rim_send[d, r, :, span:] = folds[r: r + 1]
    peers = 1
    for d in range(2):
        peers = peers + jnp.where(has_xl[d], 2, 0) + jnp.where(has_ta[d], 1, 0)
    pl.semaphore_wait(barrier, peers)
    for d in range(2):
        def go(d=d):
            for copy in rims[d]:
                copy.start()
        when(has_xl[d], go)
    bin_pair(0)
    to_other.start()
    for p in range(1, n_pairs):
        bin_pair(p)
    to_other.wait_recv()
    acc[own_row] = acc[own_row] + il_recv[...]
    for d, column in enumerate((1, own_cols)):
        def add(d=d, column=column):
            for copy in rims[d]:
                copy.wait_recv()
            for r in range(1, n_pairs + 1):
                acc[r, column: column + 1, :] += rim_recv[d, r]
            acc[own_row, column: column + 1, :] += corner_recv[d]
        when(has_xl[1 - d], add)

    halos = [remote(halo_send.at[d], halo_recv.at[d], 5 + d, {"ta": ta_at[d]}) for d in range(2)]
    for b in range(n_pairs):
        lanes = slice(b * 128, b * 128 + own_cols)
        factor = 1.0 / jnp.maximum(acc[b + 1, 1: own_cols + 1, span:], 1.0)
        for k in range(span // 128):
            part = acc[b + 1, 1: own_cols + 1, k * 128: (k + 1) * 128] * factor
            stacked[b, :, k * 128: (k + 1) * 128] = part
            if k == span // 128 - 1:
                halo_send[0, :, lanes] = part.T[128 - reach:]
            if k == 0:
                halo_send[1, :, lanes] = part.T[:reach]
    for d in range(2):
        when(has_ta[d], halos[d].start)
    for load in table_loads:
        load.wait()
    for b in range(n_pairs):
        high, low = halves(stacked[b])
        main[b] = dot(high, t_high[...]) + (dot(low, t_high[...]) + dot(high, t_low[...]))
    for d in range(2):
        def arrived(d=d):
            halos[d].wait_recv()
            halo_out[d] = halo_recv[d]

        def absent(d=d):
            halo_out[d] = jnp.zeros_like(halo_recv[d])
        when(has_ta[1 - d], arrived)
        when(jnp.logical_not(has_ta[1 - d]), absent)
    for d in range(2):
        when(has_ta[d], halos[d].wait_send)
        def sent(d=d):
            for copy in rims[d]:
                copy.wait_send()
        when(has_xl[d], sent)
    to_other.wait_send()


def finish(main, halo, t_edge, out, staged, out_sem):
    n_pairs, own_cols, width = main.shape
    writes = []
    for b in range(n_pairs):
        lanes = slice(b * 128, (b + 1) * 128)
        edges = jnp.concatenate([halo[0, :, lanes], halo[1, :, lanes]], axis=0)
        high = edges.astype(BF16).astype(F32)
        terms = jnp.concatenate([high, edges - high, high], axis=0).T[:own_cols].astype(BF16)
        staged[b] = main[b] + dot(terms, t_edge[...])
        write = pltpu.make_async_copy(staged.at[b], out.at[b], out_sem.at[b])
        write.start()
        writes.append(write)
    for write in writes:
        write.wait()


def shards(n_xl, n_ta, traces, bin_steps):
    n_rows, n_cols, span = traces.shape
    n_pairs, own_cols = n_rows // 2, n_cols // 2
    reach = TAPS // 2
    padded = (own_cols + 2 + 7) // 8 * 8
    width = span + 128
    out_span = span * P_SIZE // Q
    table = lanczos_table(span)
    t_high, t_low = split_table(table[reach:-reach])
    edge_high, edge_low = split_table(np.concatenate([table[:reach], table[-reach:]]))
    t_edge = np.concatenate([edge_high, edge_high, edge_low])
    vmem = pl.BlockSpec(memory_space=pltpu.VMEM)
    hbm = pl.BlockSpec(memory_space=pltpu.HBM)
    main, halo = pl.pallas_call(
        functools.partial(binning, n_xl, n_ta),
        out_shape=(pltpu.VMEM((n_pairs, own_cols, out_span), F32), pltpu.VMEM((2, reach, n_pairs * 128), F32)),
        in_specs=[hbm] * 4,
        out_specs=[vmem] * 2,
        scratch_shapes=[
            pltpu.VMEM((n_rows, n_cols, span), F32),
            pltpu.VMEM((2, n_rows, 8, span), F32),
            pltpu.VMEM((2, n_rows, n_cols), jnp.int32),
            pltpu.VMEM(t_high.shape, BF16),
            pltpu.VMEM(t_low.shape, BF16),
            pltpu.VMEM((2, n_pairs, 1, (n_cols + 32 + 127) // 128 * 128), jnp.int32),
            pltpu.VMEM((n_pairs + 2, padded, width), F32),
            pltpu.VMEM((n_pairs, own_cols, span), F32),
            pltpu.VMEM((2, n_pairs + 2, 1, width), F32),
            pltpu.VMEM((2, n_pairs + 2, 1, width), F32),
            pltpu.VMEM((padded, width), F32),
            pltpu.VMEM((2, 1, width), F32),
            pltpu.VMEM((2, reach, n_pairs * 128), F32),
            pltpu.VMEM((2, reach, n_pairs * 128), F32),
            pltpu.SemaphoreType.DMA((n_pairs,)),
            pltpu.SemaphoreType.DMA((2,)),
            pltpu.SemaphoreType.DMA((3,)),
            pltpu.SemaphoreType.DMA((7,)),
            pltpu.SemaphoreType.DMA((7,)),
        ],
        compiler_params=pltpu.CompilerParams(collective_id=0, has_side_effects=True, vmem_limit_bytes=24 * 2**20),
        name="binning",
    )(*[pltpu.with_memory_space_constraint(a, pltpu.HBM) for a in (traces, bin_steps, jnp.asarray(t_high), jnp.asarray(t_low))])
    return pl.pallas_call(
        finish,
        out_shape=jax.ShapeDtypeStruct((n_pairs, own_cols, out_span), F32),
        in_specs=[vmem] * 3,
        out_specs=hbm,
        scratch_shapes=[pltpu.VMEM((n_pairs, own_cols, out_span), F32), pltpu.SemaphoreType.DMA((n_pairs,))],
        compiler_params=pltpu.CompilerParams(vmem_limit_bytes=16 * 2**20),
        name="finish",
    )(main, halo, jnp.asarray(t_edge))


def solution(mesh):
    if mesh.shape["il"] != 2:
        raise ValueError("il size")
    return jax.shard_map(
        functools.partial(shards, mesh.shape["xl"], mesh.shape["ta"]),
        mesh=mesh,
        in_specs=(P("il", "xl", "ta"), P(None, "il", "xl")),
        out_specs=P("il", "xl", "ta"),
        check_vma=False,
    )
```

```python
import functools

import numpy as np
import jax
import jax.numpy as jnp
from jax import lax
from jax.experimental import pallas as pl
from jax.experimental.pallas import tpu as pltpu
from jax.sharding import PartitionSpec as P

TAPS = 16
P_SIZE = 3
Q = 2
AHEAD = 2
MESH = pl.DeviceIdType.MESH
F32, BF16 = jnp.float32, jnp.bfloat16


def lanczos_table(span):
    reach = TAPS // 2
    rows = np.arange(span + 2 * reach)[:, None] - reach
    cols = np.arange(span * P_SIZE // Q)[None, :]
    offset = (cols * Q - rows * P_SIZE).astype(np.float64) / P_SIZE
    weights = np.sinc(offset) * np.sinc(offset / reach)
    return np.where(np.abs(offset) < reach, weights, 0.0).astype(np.float32)


def split_table(table):
    high = table.astype(BF16)
    low = (table - high.astype(np.float32)).astype(BF16)
    return high, low


def halves(values):
    high = values.astype(BF16)
    low = (values - high.astype(F32)).astype(BF16)
    return high, low


def dot(a, b):
    return jnp.dot(a, b, preferred_element_type=F32)


def column_ranges(n_cols):
    split = n_cols // 2 // 16 * 16
    if split < 16 or n_cols % 16:
        raise ValueError("column count")
    ranges = []
    for start, stop in ((0, split), (split, n_cols)):
        first = start // 2 // 8 * 8
        last = (stop - 1) // 2 + 2
        ranges.append((start, stop, first, (last + 1 - first + 7) // 8 * 8))
    return ranges


def binning(n_xl, n_ta, traces, steps_hbm, t_high_hbm, t_low_hbm, main, halo_out, x, edge_x, steps, t_high, t_low, keys,
            acc, acc_ends, one_hot_low, one_hot_high, rim_send, rim_recv, il_recv, il_recv_ends, corner_recv, halo_send, halo_recv, load_sem, edge_sem, table_sem,
            send_sem, recv_sem):
    n_rows, n_cols, span = x.shape
    n_pairs = n_rows // 2
    own_cols = n_cols // 2
    reach = TAPS // 2
    il, xl, ta = lax.axis_index("il"), lax.axis_index("xl"), lax.axis_index("ta")
    other = 1 - il
    has_xl = (xl < n_xl - 1, xl > 0)
    has_ta = (ta < n_ta - 1, ta > 0)
    xl_at, ta_at = (xl + 1, xl - 1), (ta + 1, ta - 1)

    def when(condition, work):
        pl.when(condition)(work)

    def pair(p):
        return jnp.where(il == 0, n_pairs - 1 - p, p)

    step_load = pltpu.make_async_copy(steps_hbm, steps, table_sem.at[2])
    step_load.start()
    edge_loads = [pltpu.make_async_copy(traces.at[:, pl.ds(start, 8)], edge_x.at[d], edge_sem.at[d])
                  for d, start in enumerate((n_cols - 8, 0))]
    for load in edge_loads:
        load.start()
    loads = []
    for p in range(n_pairs):
        rows = pl.ds(2 * pair(p), 2)
        loads.append(pltpu.make_async_copy(traces.at[rows], x.at[rows], load_sem.at[p]))

    def load_pair(p):
        rows = pl.ds(2 * pair(p), 2)
        pltpu.make_async_copy(traces.at[rows], x.at[rows], load_sem.at[p]).start()

    pl.loop(0, n_pairs)(load_pair)
    table_loads = [pltpu.make_async_copy(t_high_hbm, t_high, table_sem.at[0]),
                   pltpu.make_async_copy(t_low_hbm, t_low, table_sem.at[1])]
    for load in table_loads:
        load.start()

    barrier = pltpu.get_barrier_semaphore()

    def greet(partner):
        pl.semaphore_signal(barrier, inc=1, device_id=partner, device_id_type=MESH)

    greet({"il": other})
    for d in range(2):
        def both(d=d):
            greet({"xl": xl_at[d]})
            greet({"il": other, "xl": xl_at[d]})
        when(has_xl[d], both)
        when(has_ta[d], lambda d=d: greet({"ta": ta_at[d]}))

    acc[...] = jnp.zeros_like(acc)
    acc_ends[...] = jnp.zeros_like(acc_ends)
    one_hots = (one_hot_low, one_hot_high)
    step_load.wait()
    ranges = column_ranges(n_cols)
    col = lax.broadcasted_iota(jnp.int32, (n_rows, n_cols), 1)
    bin_col = lax.shift_right_logical(col, 1) + steps[1] + 1
    bin_row = steps[0] + 1
    for k, (start, stop, first, height) in enumerate(ranges):
        code = bin_row * height + bin_col - first
        for p in range(n_pairs):
            keys[k, p, :, :2 * (stop - start)] = jnp.concatenate(
                [code[2 * p: 2 * p + 1, start:stop], code[2 * p + 1: 2 * p + 2, start:stop]], axis=1)

    def one_hot(key, height):
        rows = lax.broadcasted_iota(jnp.int32, (height, key.shape[1]), 0)
        return jnp.where(rows == key, 1.0, 0.0).astype(BF16)

    def totals(chosen, values):
        high, low = halves(values)
        return (dot(chosen, high) + dot(chosen, low), dot(chosen, jnp.ones((values.shape[0], 128), BF16)))

    lane = lax.broadcasted_iota(jnp.int32, (1, 128), 1)
    is_first, is_last = lane < reach, lane >= 128 - reach

    def pair_values(at, start, stop, samples):
        return jnp.concatenate([x[2 * at, start:stop, samples], x[2 * at + 1, start:stop, samples]], axis=0)

    def bin_edges(p):
        at = pair(p)
        loads[p].wait()
        for k, (start, stop, first, height) in enumerate(ranges):
            chosen = one_hot(keys[k, at][:, :2 * (stop - start)], 3 * height)
            one_hots[k][at] = chosen
            values = jnp.where(lane < 64, pair_values(at, start, stop, slice(0, 128)),
                               pair_values(at, start, stop, slice(span - 128, span)))
            high = values.astype(BF16)
            low = jnp.where(is_first | is_last, values - high.astype(F32), 1.0).astype(BF16)
            sums = dot(chosen, jnp.concatenate([high, low], axis=1))
            ends = jnp.where(is_first | is_last, sums[:, :128], 0.0) + sums[:, 128:]
            for r in range(3):
                acc_ends[at + r, first: first + height, :] += ends[r * height: (r + 1) * height]

    def bin_pair(p):
        at = pair(p)
        for k, (start, stop, first, height) in enumerate(ranges):
            chosen = one_hots[k][at]
            high, low = halves(pair_values(at, start, stop, slice(0, span)))
            sums = dot(chosen, high) + dot(chosen, low)
            for r in range(3):
                acc[at + r, first: first + height, :] += sums[r * height: (r + 1) * height]

    def remote(src, dst, slot, partner):
        return pltpu.make_async_remote_copy(src_ref=src, dst_ref=dst, send_sem=send_sem.at[slot],
                                            recv_sem=recv_sem.at[slot], device_id=partner, device_id_type=MESH)

    rim_row = jnp.where(il == 0, n_pairs + 1, 0)
    own_row = jnp.where(il == 0, n_pairs, 1)
    to_other = remote(acc.at[rim_row], il_recv, 0, {"il": other})
    ends_to_other = remote(acc_ends.at[rim_row], il_recv_ends, 7, {"il": other})
    rims = [(remote(rim_send.at[d], rim_recv.at[d], 1 + d, {"xl": xl_at[d]}),
             remote(rim_send.at[d, rim_row], corner_recv.at[d], 3 + d, {"il": other, "xl": xl_at[d]}))
            for d in range(2)]

    row = lax.broadcasted_iota(jnp.int32, (n_rows, n_cols), 0)
    rim_bin = bin_row + lax.shift_right_logical(row, 1)
    for load in edge_loads:
        load.wait()
    for d, (start, column) in enumerate(((n_cols - 8, own_cols + 1), (0, 0))):
        target = jnp.where(bin_col == column, rim_bin, -1)
        key = jnp.concatenate([target[i: i + 1, start: start + 8] for i in range(n_rows)], axis=1)
        sums, folds = totals(one_hot(key, (n_pairs + 2 + 7) // 8 * 8), edge_x[d].reshape(n_rows * 8, span))
        for r in range(n_pairs + 2):
            rim_send[d, r, :, :span] = sums[r: r + 1]
            rim_send[d, r, :, span:] = jnp.where(is_first, sums[r: r + 1, :128], jnp.where(
                is_last, sums[r: r + 1, span - 128:], folds[r: r + 1]))
    peers = 1
    for d in range(2):
        peers = peers + jnp.where(has_xl[d], 2, 0) + jnp.where(has_ta[d], 1, 0)
    pl.semaphore_wait(barrier, peers)
    for d in range(2):
        def go(d=d):
            for copy in rims[d]:
                copy.start()
        when(has_xl[d], go)
    bin_edges(0)
    ends_to_other.start()
    for p in range(1, n_pairs):
        bin_edges(p)
    for p in range(AHEAD):
        bin_pair(p)
        if p == 0:
            to_other.start()
    ends_to_other.wait_recv()
    acc_ends[own_row] = acc_ends[own_row] + il_recv_ends[...]
    for d, column in enumerate((1, own_cols)):
        def add_ends(d=d, column=column):
            for copy in rims[d]:
                copy.wait_recv()
            for r in range(1, n_pairs + 1):
                acc_ends[r, column: column + 1, :] += rim_recv[d, r, :, span:]
            acc_ends[own_row, column: column + 1, :] += corner_recv[d, :, span:]
        when(has_xl[1 - d], add_ends)

    halos = [remote(halo_send.at[d], halo_recv.at[d], 5 + d, {"ta": ta_at[d]}) for d in range(2)]
    for b in range(n_pairs):
        lanes = slice(b * 128, b * 128 + own_cols)
        ends = acc_ends[b + 1, 1: own_cols + 1, :].T
        factor = 1.0 / jnp.maximum(ends[64:64 + reach], 1.0)
        halo_send[0, :, lanes] = ends[128 - reach:] * factor
        halo_send[1, :, lanes] = ends[:reach] * factor
    for d in range(2):
        when(has_ta[d], halos[d].start)

    for p in range(AHEAD, n_pairs):
        bin_pair(p)
        if p == 0:
            to_other.start()
    to_other.wait_recv()
    acc[own_row] = acc[own_row] + il_recv[...]
    for d, column in enumerate((1, own_cols)):
        def add(d=d, column=column):
            for r in range(1, n_pairs + 1):
                acc[r, column: column + 1, :] += rim_recv[d, r, :, :span]
            acc[own_row, column: column + 1, :] += corner_recv[d, :, :span]
        when(has_xl[1 - d], add)
    for load in table_loads:
        load.wait()
    for b in range(n_pairs):
        fold = jnp.broadcast_to(acc_ends[b + 1, 1: own_cols + 1, 64:65], (own_cols, 128))
        factor = 1.0 / jnp.maximum(fold, 1.0)
        sums = acc[b + 1, 1: own_cols + 1, :]
        high, low = halves(sums * jnp.concatenate([factor] * (span // 128), axis=1))
        main[b] = dot(high, t_high[...]) + (dot(low, t_high[...]) + dot(high, t_low[...]))
    for d in range(2):
        def arrived(d=d):
            halos[d].wait_recv()
            halo_out[d] = halo_recv[d]

        def absent(d=d):
            halo_out[d] = jnp.zeros_like(halo_recv[d])
        when(has_ta[1 - d], arrived)
        when(jnp.logical_not(has_ta[1 - d]), absent)
    for d in range(2):
        when(has_ta[d], halos[d].wait_send)
        def sent(d=d):
            for copy in rims[d]:
                copy.wait_send()
        when(has_xl[d], sent)
    to_other.wait_send()
    ends_to_other.wait_send()


def finish(main, halo, t_edge, out, staged, out_sem):
    n_pairs, own_cols, width = main.shape
    writes = []
    for b in range(n_pairs):
        lanes = slice(b * 128, (b + 1) * 128)
        edges = jnp.concatenate([halo[0, :, lanes], halo[1, :, lanes]], axis=0)
        high = edges.astype(BF16).astype(F32)
        terms = jnp.concatenate([high, edges - high, high], axis=0).T[:own_cols].astype(BF16)
        staged[b] = main[b] + dot(terms, t_edge[...])
        write = pltpu.make_async_copy(staged.at[b], out.at[b], out_sem.at[b])
        write.start()
        writes.append(write)
    for write in writes:
        write.wait()


def shards(n_xl, n_ta, traces, bin_steps):
    n_rows, n_cols, span = traces.shape
    n_pairs, own_cols = n_rows // 2, n_cols // 2
    reach = TAPS // 2
    padded = (own_cols + 2 + 7) // 8 * 8
    width = span + 128
    out_span = span * P_SIZE // Q
    table = lanczos_table(span)
    t_high, t_low = split_table(table[reach:-reach])
    edge_high, edge_low = split_table(np.concatenate([table[:reach], table[-reach:]]))
    t_edge = np.concatenate([edge_high, edge_high, edge_low])
    vmem = pl.BlockSpec(memory_space=pltpu.VMEM)
    hbm = pl.BlockSpec(memory_space=pltpu.HBM)
    main, halo = pl.pallas_call(
        functools.partial(binning, n_xl, n_ta),
        out_shape=(pltpu.VMEM((n_pairs, own_cols, out_span), F32), pltpu.VMEM((2, reach, n_pairs * 128), F32)),
        in_specs=[hbm] * 4,
        out_specs=[vmem] * 2,
        scratch_shapes=[
            pltpu.VMEM((n_rows, n_cols, span), F32),
            pltpu.VMEM((2, n_rows, 8, span), F32),
            pltpu.VMEM((2, n_rows, n_cols), jnp.int32),
            pltpu.VMEM(t_high.shape, BF16),
            pltpu.VMEM(t_low.shape, BF16),
            pltpu.VMEM((2, n_pairs, 1, (n_cols + 32 + 127) // 128 * 128), jnp.int32),
            pltpu.VMEM((n_pairs + 2, padded, span), F32),
            pltpu.VMEM((n_pairs + 2, padded, 128), F32),
            *[pltpu.VMEM((n_pairs, 3 * height, 2 * (stop - start)), BF16)
              for start, stop, _, height in column_ranges(n_cols)],
            pltpu.VMEM((2, n_pairs + 2, 1, width), F32),
            pltpu.VMEM((2, n_pairs + 2, 1, width), F32),
            pltpu.VMEM((padded, span), F32),
            pltpu.VMEM((padded, 128), F32),
            pltpu.VMEM((2, 1, width), F32),
            pltpu.VMEM((2, reach, n_pairs * 128), F32),
            pltpu.VMEM((2, reach, n_pairs * 128), F32),
            pltpu.SemaphoreType.DMA((n_pairs,)),
            pltpu.SemaphoreType.DMA((2,)),
            pltpu.SemaphoreType.DMA((3,)),
            pltpu.SemaphoreType.DMA((8,)),
            pltpu.SemaphoreType.DMA((8,)),
        ],
        compiler_params=pltpu.CompilerParams(collective_id=0, has_side_effects=True, vmem_limit_bytes=24 * 2**20),
        name="binning",
    )(*[pltpu.with_memory_space_constraint(a, pltpu.HBM) for a in (traces, bin_steps, jnp.asarray(t_high), jnp.asarray(t_low))])
    return pl.pallas_call(
        finish,
        out_shape=jax.ShapeDtypeStruct((n_pairs, own_cols, out_span), F32),
        in_specs=[vmem] * 3,
        out_specs=hbm,
        scratch_shapes=[pltpu.VMEM((n_pairs, own_cols, out_span), F32), pltpu.SemaphoreType.DMA((n_pairs,))],
        compiler_params=pltpu.CompilerParams(vmem_limit_bytes=16 * 2**20),
        name="finish",
    )(main, halo, jnp.asarray(t_edge))


def solution(mesh):
    if mesh.shape["il"] != 2:
        raise ValueError("il size")
    return jax.shard_map(
        functools.partial(shards, mesh.shape["xl"], mesh.shape["ta"]),
        mesh=mesh,
        in_specs=(P("il", "xl", "ta"), P(None, "il", "xl")),
        out_specs=P("il", "xl", "ta"),
        check_vma=False,
    )
```

```python
import functools

import numpy as np
import jax
import jax.numpy as jnp
from jax import lax
from jax.experimental import pallas as pl
from jax.experimental.pallas import tpu as pltpu
from jax.sharding import PartitionSpec as P

TAPS = 16
P_SIZE = 3
Q = 2
MESH = pl.DeviceIdType.MESH
F32, BF16 = jnp.float32, jnp.bfloat16


def lanczos_table(span):
    reach = TAPS // 2
    rows = np.arange(span + 2 * reach)[:, None] - reach
    cols = np.arange(span * P_SIZE // Q)[None, :]
    offset = (cols * Q - rows * P_SIZE).astype(np.float64) / P_SIZE
    weights = np.sinc(offset) * np.sinc(offset / reach)
    return np.where(np.abs(offset) < reach, weights, 0.0).astype(np.float32)


def split_table(table):
    high = table.astype(BF16)
    low = (table - high.astype(np.float32)).astype(BF16)
    return high, low


def halves(values):
    high = values.astype(BF16)
    low = (values - high.astype(F32)).astype(BF16)
    return high, low


def dot(a, b):
    return jnp.dot(a, b, preferred_element_type=F32)


def column_ranges(n_cols):
    split = n_cols // 2 // 16 * 16
    if split < 16 or n_cols % 16:
        raise ValueError("column count")
    ranges = []
    for start, stop in ((0, split), (split, n_cols)):
        first = start // 2 // 8 * 8
        last = (stop - 1) // 2 + 2
        ranges.append((start, stop, first, (last + 1 - first + 7) // 8 * 8))
    return ranges


def binning(n_xl, n_ta, traces, steps_hbm, t_high_hbm, t_low_hbm, main, halo_out, x, edge_x, steps, t_high, t_low, keys,
            acc, stacked, rim_send, rim_recv, il_recv, corner_recv, halo_send, halo_recv, load_sem, edge_sem, table_sem,
            send_sem, recv_sem):
    n_rows, n_cols, span = x.shape
    n_pairs = n_rows // 2
    own_cols = n_cols // 2
    reach = TAPS // 2
    il, xl, ta = lax.axis_index("il"), lax.axis_index("xl"), lax.axis_index("ta")
    other = 1 - il
    has_xl = (xl < n_xl - 1, xl > 0)
    has_ta = (ta < n_ta - 1, ta > 0)
    xl_at, ta_at = (xl + 1, xl - 1), (ta + 1, ta - 1)

    def when(condition, work):
        pl.when(condition)(work)

    def pair(p):
        return jnp.where(il == 0, n_pairs - 1 - p, p)

    step_load = pltpu.make_async_copy(steps_hbm, steps, table_sem.at[2])
    step_load.start()
    edge_loads = [pltpu.make_async_copy(traces.at[:, pl.ds(start, 8)], edge_x.at[d], edge_sem.at[d])
                  for d, start in enumerate((n_cols - 8, 0))]
    for load in edge_loads:
        load.start()
    loads = []
    for p in range(n_pairs):
        rows = pl.ds(2 * pair(p), 2)
        loads.append(pltpu.make_async_copy(traces.at[rows], x.at[rows], load_sem.at[p]))

    def load_pair(p):
        rows = pl.ds(2 * pair(p), 2)
        pltpu.make_async_copy(traces.at[rows], x.at[rows], load_sem.at[p]).start()

    pl.loop(0, n_pairs)(load_pair)
    table_loads = [pltpu.make_async_copy(t_high_hbm, t_high, table_sem.at[0]),
                   pltpu.make_async_copy(t_low_hbm, t_low, table_sem.at[1])]
    for load in table_loads:
        load.start()

    barrier = pltpu.get_barrier_semaphore()

    def greet(partner):
        pl.semaphore_signal(barrier, inc=1, device_id=partner, device_id_type=MESH)

    greet({"il": other})
    for d in range(2):
        def both(d=d):
            greet({"xl": xl_at[d]})
            greet({"il": other, "xl": xl_at[d]})
        when(has_xl[d], both)
        when(has_ta[d], lambda d=d: greet({"ta": ta_at[d]}))

    acc[...] = jnp.zeros_like(acc)
    step_load.wait()
    ranges = column_ranges(n_cols)
    col = lax.broadcasted_iota(jnp.int32, (n_rows, n_cols), 1)
    bin_col = lax.shift_right_logical(col, 1) + steps[1] + 1
    bin_row = steps[0] + 1
    for k, (start, stop, first, height) in enumerate(ranges):
        code = bin_row * height + bin_col - first
        for p in range(n_pairs):
            keys[k, p, :, :2 * (stop - start)] = jnp.concatenate(
                [code[2 * p: 2 * p + 1, start:stop], code[2 * p + 1: 2 * p + 2, start:stop]], axis=1)

    def one_hot(key, height):
        rows = lax.broadcasted_iota(jnp.int32, (height, key.shape[1]), 0)
        return jnp.where(rows == key, 1.0, 0.0).astype(BF16)

    def totals(chosen, values):
        high, low = halves(values)
        return (dot(chosen, high) + dot(chosen, low), dot(chosen, jnp.ones((values.shape[0], 128), BF16)))

    def bin_pair(p):
        at = pair(p)
        loads[p].wait()
        for k, (start, stop, first, height) in enumerate(ranges):
            key = keys[k, at][:, :2 * (stop - start)]
            values = jnp.concatenate([x[2 * at, start:stop, :], x[2 * at + 1, start:stop, :]], axis=0)
            sums, folds = totals(one_hot(key, 3 * height), values)
            for r in range(3):
                acc[at + r, first: first + height, :span] += sums[r * height: (r + 1) * height]
                acc[at + r, first: first + height, span:] += folds[r * height: (r + 1) * height]

    def remote(src, dst, slot, partner):
        return pltpu.make_async_remote_copy(src_ref=src, dst_ref=dst, send_sem=send_sem.at[slot],
                                            recv_sem=recv_sem.at[slot], device_id=partner, device_id_type=MESH)

    rim_row = jnp.where(il == 0, n_pairs + 1, 0)
    own_row = jnp.where(il == 0, n_pairs, 1)
    to_other = remote(acc.at[rim_row], il_recv, 0, {"il": other})
    rims = [(remote(rim_send.at[d], rim_recv.at[d], 1 + d, {"xl": xl_at[d]}),
             remote(rim_send.at[d, rim_row], corner_recv.at[d], 3 + d, {"il": other, "xl": xl_at[d]}))
            for d in range(2)]

    row = lax.broadcasted_iota(jnp.int32, (n_rows, n_cols), 0)
    rim_bin = bin_row + lax.shift_right_logical(row, 1)
    for load in edge_loads:
        load.wait()
    for d, (start, column) in enumerate(((n_cols - 8, own_cols + 1), (0, 0))):
        target = jnp.where(bin_col == column, rim_bin, -1)
        key = jnp.concatenate([target[i: i + 1, start: start + 8] for i in range(n_rows)], axis=1)
        sums, folds = totals(one_hot(key, (n_pairs + 2 + 7) // 8 * 8), edge_x[d].reshape(n_rows * 8, span))
        for r in range(n_pairs + 2):
            rim_send[d, r, :, :span] = sums[r: r + 1]
            rim_send[d, r, :, span:] = folds[r: r + 1]
    peers = 1
    for d in range(2):
        peers = peers + jnp.where(has_xl[d], 2, 0) + jnp.where(has_ta[d], 1, 0)
    pl.semaphore_wait(barrier, peers)
    for d in range(2):
        def go(d=d):
            for copy in rims[d]:
                copy.start()
        when(has_xl[d], go)
    bin_pair(0)
    to_other.start()
    for p in range(1, n_pairs):
        bin_pair(p)
    to_other.wait_recv()
    acc[own_row] = acc[own_row] + il_recv[...]
    for d, column in enumerate((1, own_cols)):
        def add(d=d, column=column):
            for copy in rims[d]:
                copy.wait_recv()
            for r in range(1, n_pairs + 1):
                acc[r, column: column + 1, :] += rim_recv[d, r]
            acc[own_row, column: column + 1, :] += corner_recv[d]
        when(has_xl[1 - d], add)

    halos = [remote(halo_send.at[d], halo_recv.at[d], 5 + d, {"ta": ta_at[d]}) for d in range(2)]
    for b in range(n_pairs):
        lanes = slice(b * 128, b * 128 + own_cols)
        factor = 1.0 / jnp.maximum(acc[b + 1, 1: own_cols + 1, span:], 1.0)
        for k in range(span // 128):
            part = acc[b + 1, 1: own_cols + 1, k * 128: (k + 1) * 128] * factor
            stacked[b, :, k * 128: (k + 1) * 128] = part
            if k == span // 128 - 1:
                halo_send[0, :, lanes] = part.T[128 - reach:]
            if k == 0:
                halo_send[1, :, lanes] = part.T[:reach]
    for d in range(2):
        when(has_ta[d], halos[d].start)
    for load in table_loads:
        load.wait()
    for b in range(n_pairs):
        high, low = halves(stacked[b])
        main[b] = dot(high, t_high[...]) + (dot(low, t_high[...]) + dot(high, t_low[...]))
    for d in range(2):
        def arrived(d=d):
            halos[d].wait_recv()
            halo_out[d] = halo_recv[d]

        def absent(d=d):
            halo_out[d] = jnp.zeros_like(halo_recv[d])
        when(has_ta[1 - d], arrived)
        when(jnp.logical_not(has_ta[1 - d]), absent)
    for d in range(2):
        when(has_ta[d], halos[d].wait_send)
        def sent(d=d):
            for copy in rims[d]:
                copy.wait_send()
        when(has_xl[d], sent)
    to_other.wait_send()


def finish(main, halo, t_edge, out, staged, out_sem):
    n_pairs, own_cols, width = main.shape
    inner = pl.ds(128, width - 256)
    writes = [pltpu.make_async_copy(main.at[:, :, inner], out.at[:, :, inner], out_sem.at[n_pairs, 0])]
    writes[0].start()
    for b in range(n_pairs):
        lanes = slice(b * 128, (b + 1) * 128)
        edges = jnp.concatenate([halo[0, :, lanes], halo[1, :, lanes]], axis=0)
        high = edges.astype(BF16).astype(F32)
        terms = jnp.concatenate([high, edges - high, high], axis=0).T[:own_cols].astype(BF16)
        ends = dot(terms, t_edge[...])
        for d, start in enumerate((0, width - 128)):
            staged[b, d] = main[b, :, start: start + 128] + ends[:, d * 128: (d + 1) * 128]
            write = pltpu.make_async_copy(staged.at[b, d], out.at[b, :, pl.ds(start, 128)], out_sem.at[b, d])
            write.start()
            writes.append(write)
    for write in writes:
        write.wait()


def shards(n_xl, n_ta, traces, bin_steps):
    n_rows, n_cols, span = traces.shape
    n_pairs, own_cols = n_rows // 2, n_cols // 2
    reach = TAPS // 2
    padded = (own_cols + 2 + 7) // 8 * 8
    width = span + 128
    out_span = span * P_SIZE // Q
    table = lanczos_table(span)
    t_high, t_low = split_table(table[reach:-reach])
    edge_high, edge_low = split_table(np.concatenate([table[:reach], table[-reach:]]))
    t_edge = np.concatenate([edge_high, edge_high, edge_low])
    t_edge = np.concatenate([t_edge[:, :128], t_edge[:, -128:]], axis=1)
    if out_span < 384:
        raise ValueError("sample count")
    vmem = pl.BlockSpec(memory_space=pltpu.VMEM)
    hbm = pl.BlockSpec(memory_space=pltpu.HBM)
    main, halo = pl.pallas_call(
        functools.partial(binning, n_xl, n_ta),
        out_shape=(pltpu.VMEM((n_pairs, own_cols, out_span), F32), pltpu.VMEM((2, reach, n_pairs * 128), F32)),
        in_specs=[hbm] * 4,
        out_specs=[vmem] * 2,
        scratch_shapes=[
            pltpu.VMEM((n_rows, n_cols, span), F32),
            pltpu.VMEM((2, n_rows, 8, span), F32),
            pltpu.VMEM((2, n_rows, n_cols), jnp.int32),
            pltpu.VMEM(t_high.shape, BF16),
            pltpu.VMEM(t_low.shape, BF16),
            pltpu.VMEM((2, n_pairs, 1, (n_cols + 32 + 127) // 128 * 128), jnp.int32),
            pltpu.VMEM((n_pairs + 2, padded, width), F32),
            pltpu.VMEM((n_pairs, own_cols, span), F32),
            pltpu.VMEM((2, n_pairs + 2, 1, width), F32),
            pltpu.VMEM((2, n_pairs + 2, 1, width), F32),
            pltpu.VMEM((padded, width), F32),
            pltpu.VMEM((2, 1, width), F32),
            pltpu.VMEM((2, reach, n_pairs * 128), F32),
            pltpu.VMEM((2, reach, n_pairs * 128), F32),
            pltpu.SemaphoreType.DMA((n_pairs,)),
            pltpu.SemaphoreType.DMA((2,)),
            pltpu.SemaphoreType.DMA((3,)),
            pltpu.SemaphoreType.DMA((7,)),
            pltpu.SemaphoreType.DMA((7,)),
        ],
        compiler_params=pltpu.CompilerParams(collective_id=0, has_side_effects=True, vmem_limit_bytes=24 * 2**20),
        name="binning",
    )(*[pltpu.with_memory_space_constraint(a, pltpu.HBM) for a in (traces, bin_steps, jnp.asarray(t_high), jnp.asarray(t_low))])
    return pl.pallas_call(
        finish,
        out_shape=jax.ShapeDtypeStruct((n_pairs, own_cols, out_span), F32),
        in_specs=[vmem] * 3,
        out_specs=hbm,
        scratch_shapes=[pltpu.VMEM((n_pairs, 2, own_cols, 128), F32), pltpu.SemaphoreType.DMA((n_pairs + 1, 2))],
        compiler_params=pltpu.CompilerParams(vmem_limit_bytes=16 * 2**20),
        name="finish",
    )(main, halo, jnp.asarray(t_edge))


def solution(mesh):
    if mesh.shape["il"] != 2:
        raise ValueError("il size")
    return jax.shard_map(
        functools.partial(shards, mesh.shape["xl"], mesh.shape["ta"]),
        mesh=mesh,
        in_specs=(P("il", "xl", "ta"), P(None, "il", "xl")),
        out_specs=P("il", "xl", "ta"),
        check_vma=False,
    )
```

```python
import functools

import numpy as np
import jax
import jax.numpy as jnp
from jax import lax
from jax.experimental import pallas as pl
from jax.experimental.pallas import tpu as pltpu
from jax.sharding import PartitionSpec as P

TAPS = 16
P_SIZE = 3
Q = 2
AHEAD = 2
MESH = pl.DeviceIdType.MESH
F32, BF16 = jnp.float32, jnp.bfloat16


def lanczos_table(span):
    reach = TAPS // 2
    rows = np.arange(span + 2 * reach)[:, None] - reach
    cols = np.arange(span * P_SIZE // Q)[None, :]
    offset = (cols * Q - rows * P_SIZE).astype(np.float64) / P_SIZE
    weights = np.sinc(offset) * np.sinc(offset / reach)
    return np.where(np.abs(offset) < reach, weights, 0.0).astype(np.float32)


def split_table(table):
    high = table.astype(BF16)
    low = (table - high.astype(np.float32)).astype(BF16)
    return high, low


def halves(values):
    high = values.astype(BF16)
    low = (values - high.astype(F32)).astype(BF16)
    return high, low


def dot(a, b):
    return jnp.dot(a, b, preferred_element_type=F32)


def column_ranges(n_cols):
    split = n_cols // 2 // 16 * 16
    if split < 16 or n_cols % 16:
        raise ValueError("column count")
    ranges = []
    for start, stop in ((0, split), (split, n_cols)):
        first = start // 2 // 8 * 8
        last = (stop - 1) // 2 + 2
        ranges.append((start, stop, first, (last + 1 - first + 7) // 8 * 8))
    return ranges


def binning(n_xl, n_ta, traces, steps_hbm, t_high_hbm, t_low_hbm, main, halo_out, x, edge_x, steps, t_high, t_low, keys,
            acc, acc_ends, one_hot_low, one_hot_high, rim_send, rim_recv, il_recv, il_recv_ends, corner_recv, halo_send, halo_recv, load_sem, edge_sem, table_sem,
            send_sem, recv_sem):
    n_rows, n_cols, span = x.shape
    n_pairs = n_rows // 2
    own_cols = n_cols // 2
    reach = TAPS // 2
    il, xl, ta = lax.axis_index("il"), lax.axis_index("xl"), lax.axis_index("ta")
    other = 1 - il
    has_xl = (xl < n_xl - 1, xl > 0)
    has_ta = (ta < n_ta - 1, ta > 0)
    xl_at, ta_at = (xl + 1, xl - 1), (ta + 1, ta - 1)

    def when(condition, work):
        pl.when(condition)(work)

    def pair(p):
        return jnp.where(il == 0, n_pairs - 1 - p, p)

    step_load = pltpu.make_async_copy(steps_hbm, steps, table_sem.at[2])
    step_load.start()
    edge_loads = [pltpu.make_async_copy(traces.at[:, pl.ds(start, 8)], edge_x.at[d], edge_sem.at[d])
                  for d, start in enumerate((n_cols - 8, 0))]
    for load in edge_loads:
        load.start()
    loads = []
    for p in range(n_pairs):
        rows = pl.ds(2 * pair(p), 2)
        loads.append(pltpu.make_async_copy(traces.at[rows], x.at[rows], load_sem.at[p]))

    barrier = pltpu.get_barrier_semaphore()

    def greet(partner):
        pl.semaphore_signal(barrier, inc=1, device_id=partner, device_id_type=MESH)

    greet({"il": other})
    for d in range(2):
        def both(d=d):
            greet({"xl": xl_at[d]})
            greet({"il": other, "xl": xl_at[d]})
        when(has_xl[d], both)
        when(has_ta[d], lambda d=d: greet({"ta": ta_at[d]}))

    def load_pair(p):
        rows = pl.ds(2 * pair(p), 2)
        pltpu.make_async_copy(traces.at[rows], x.at[rows], load_sem.at[p]).start()

    pl.loop(0, n_pairs)(load_pair)
    table_loads = [pltpu.make_async_copy(t_high_hbm, t_high, table_sem.at[0]),
                   pltpu.make_async_copy(t_low_hbm, t_low, table_sem.at[1])]
    for load in table_loads:
        load.start()

    acc[...] = jnp.zeros_like(acc)
    acc_ends[...] = jnp.zeros_like(acc_ends)
    one_hots = (one_hot_low, one_hot_high)
    step_load.wait()
    ranges = column_ranges(n_cols)
    col = lax.broadcasted_iota(jnp.int32, (n_rows, n_cols), 1)
    bin_col = lax.shift_right_logical(col, 1) + steps[1] + 1
    bin_row = steps[0] + 1
    for k, (start, stop, first, height) in enumerate(ranges):
        code = bin_row * height + bin_col - first
        for p in range(n_pairs):
            keys[k, p, :, :2 * (stop - start)] = jnp.concatenate(
                [code[2 * p: 2 * p + 1, start:stop], code[2 * p + 1: 2 * p + 2, start:stop]], axis=1)

    def one_hot(key, height):
        rows = lax.broadcasted_iota(jnp.int32, (height, key.shape[1]), 0)
        return jnp.where(rows == key, 1.0, 0.0).astype(BF16)

    def totals(chosen, values):
        high, low = halves(values)
        return (dot(chosen, high) + dot(chosen, low), dot(chosen, jnp.ones((values.shape[0], 128), BF16)))

    lane = lax.broadcasted_iota(jnp.int32, (1, 128), 1)
    is_first, is_last = lane < reach, lane >= 128 - reach

    def pair_values(at, start, stop, samples):
        return jnp.concatenate([x[2 * at, start:stop, samples], x[2 * at + 1, start:stop, samples]], axis=0)

    def bin_edges(p):
        at = pair(p)
        loads[p].wait()
        for k, (start, stop, first, height) in enumerate(ranges):
            chosen = one_hot(keys[k, at][:, :2 * (stop - start)], 3 * height)
            one_hots[k][at] = chosen
            values = jnp.where(lane < 64, pair_values(at, start, stop, slice(0, 128)),
                               pair_values(at, start, stop, slice(span - 128, span)))
            high = values.astype(BF16)
            low = jnp.where(is_first | is_last, values - high.astype(F32), 1.0).astype(BF16)
            sums = dot(chosen, jnp.concatenate([high, low], axis=1))
            ends = jnp.where(is_first | is_last, sums[:, :128], 0.0) + sums[:, 128:]
            for r in range(3):
                acc_ends[at + r, first: first + height, :] += ends[r * height: (r + 1) * height]

    def bin_pair(p):
        at = pair(p)
        for k, (start, stop, first, height) in enumerate(ranges):
            chosen = one_hots[k][at]
            high, low = halves(pair_values(at, start, stop, slice(0, span)))
            sums = dot(chosen, high) + dot(chosen, low)
            for r in range(3):
                acc[at + r, first: first + height, :] += sums[r * height: (r + 1) * height]

    def remote(src, dst, slot, partner):
        return pltpu.make_async_remote_copy(src_ref=src, dst_ref=dst, send_sem=send_sem.at[slot],
                                            recv_sem=recv_sem.at[slot], device_id=partner, device_id_type=MESH)

    rim_row = jnp.where(il == 0, n_pairs + 1, 0)
    own_row = jnp.where(il == 0, n_pairs, 1)
    to_other = remote(acc.at[rim_row], il_recv, 0, {"il": other})
    ends_to_other = remote(acc_ends.at[rim_row], il_recv_ends, 7, {"il": other})
    rims = [(remote(rim_send.at[d], rim_recv.at[d], 1 + d, {"xl": xl_at[d]}),
             remote(rim_send.at[d, rim_row], corner_recv.at[d], 3 + d, {"il": other, "xl": xl_at[d]}))
            for d in range(2)]

    row = lax.broadcasted_iota(jnp.int32, (n_rows, n_cols), 0)
    rim_bin = bin_row + lax.shift_right_logical(row, 1)
    for load in edge_loads:
        load.wait()
    for d, (start, column) in enumerate(((n_cols - 8, own_cols + 1), (0, 0))):
        target = jnp.where(bin_col == column, rim_bin, -1)
        key = jnp.concatenate([target[i: i + 1, start: start + 8] for i in range(n_rows)], axis=1)
        sums, folds = totals(one_hot(key, (n_pairs + 2 + 7) // 8 * 8), edge_x[d].reshape(n_rows * 8, span))
        for r in range(n_pairs + 2):
            rim_send[d, r, :, :span] = sums[r: r + 1]
            rim_send[d, r, :, span:] = jnp.where(is_first, sums[r: r + 1, :128], jnp.where(
                is_last, sums[r: r + 1, span - 128:], folds[r: r + 1]))
    peers = 1
    for d in range(2):
        peers = peers + jnp.where(has_xl[d], 2, 0) + jnp.where(has_ta[d], 1, 0)
    pl.semaphore_wait(barrier, peers)
    for d in range(2):
        def go(d=d):
            for copy in rims[d]:
                copy.start()
        when(has_xl[d], go)
    bin_edges(0)
    ends_to_other.start()
    for p in range(1, n_pairs):
        bin_edges(p)
    for p in range(AHEAD):
        bin_pair(p)
        if p == 0:
            to_other.start()
    ends_to_other.wait_recv()
    acc_ends[own_row] = acc_ends[own_row] + il_recv_ends[...]
    for d, column in enumerate((1, own_cols)):
        def add_ends(d=d, column=column):
            for copy in rims[d]:
                copy.wait_recv()
            for r in range(1, n_pairs + 1):
                acc_ends[r, column: column + 1, :] += rim_recv[d, r, :, span:]
            acc_ends[own_row, column: column + 1, :] += corner_recv[d, :, span:]
        when(has_xl[1 - d], add_ends)

    halos = [remote(halo_send.at[d], halo_recv.at[d], 5 + d, {"ta": ta_at[d]}) for d in range(2)]
    for b in range(n_pairs):
        lanes = slice(b * 128, b * 128 + own_cols)
        ends = acc_ends[b + 1, 1: own_cols + 1, :].T
        factor = 1.0 / jnp.maximum(ends[64:64 + reach], 1.0)
        halo_send[0, :, lanes] = ends[128 - reach:] * factor
        halo_send[1, :, lanes] = ends[:reach] * factor
    for d in range(2):
        when(has_ta[d], halos[d].start)

    for p in range(AHEAD, n_pairs):
        bin_pair(p)
        if p == 0:
            to_other.start()
    to_other.wait_recv()
    acc[own_row] = acc[own_row] + il_recv[...]
    for d, column in enumerate((1, own_cols)):
        def add(d=d, column=column):
            for r in range(1, n_pairs + 1):
                acc[r, column: column + 1, :] += rim_recv[d, r, :, :span]
            acc[own_row, column: column + 1, :] += corner_recv[d, :, :span]
        when(has_xl[1 - d], add)
    for load in table_loads:
        load.wait()
    for b in range(n_pairs):
        fold = jnp.broadcast_to(acc_ends[b + 1, 1: own_cols + 1, 64:65], (own_cols, 128))
        factor = 1.0 / jnp.maximum(fold, 1.0)
        sums = acc[b + 1, 1: own_cols + 1, :]
        high, low = halves(sums * jnp.concatenate([factor] * (span // 128), axis=1))
        main[b] = dot(high, t_high[...]) + (dot(low, t_high[...]) + dot(high, t_low[...]))
    for d in range(2):
        def arrived(d=d):
            halos[d].wait_recv()
            halo_out[d] = halo_recv[d]

        def absent(d=d):
            halo_out[d] = jnp.zeros_like(halo_recv[d])
        when(has_ta[1 - d], arrived)
        when(jnp.logical_not(has_ta[1 - d]), absent)
    for d in range(2):
        when(has_ta[d], halos[d].wait_send)
        def sent(d=d):
            for copy in rims[d]:
                copy.wait_send()
        when(has_xl[d], sent)
    to_other.wait_send()
    ends_to_other.wait_send()


def finish(main, halo, t_edge, out, staged, out_sem):
    n_pairs, own_cols, width = main.shape
    inner = pl.ds(128, width - 256)
    writes = [pltpu.make_async_copy(main.at[:, :, inner], out.at[:, :, inner], out_sem.at[n_pairs, 0])]
    writes[0].start()
    for b in range(n_pairs):
        lanes = slice(b * 128, (b + 1) * 128)
        edges = jnp.concatenate([halo[0, :, lanes], halo[1, :, lanes]], axis=0)
        high = edges.astype(BF16).astype(F32)
        terms = jnp.concatenate([high, edges - high, high], axis=0).T[:own_cols].astype(BF16)
        ends = dot(terms, t_edge[...])
        for d, start in enumerate((0, width - 128)):
            staged[b, d] = main[b, :, start: start + 128] + ends[:, d * 128: (d + 1) * 128]
            write = pltpu.make_async_copy(staged.at[b, d], out.at[b, :, pl.ds(start, 128)], out_sem.at[b, d])
            write.start()
            writes.append(write)
    for write in writes:
        write.wait()


def shards(n_xl, n_ta, traces, bin_steps):
    n_rows, n_cols, span = traces.shape
    n_pairs, own_cols = n_rows // 2, n_cols // 2
    reach = TAPS // 2
    padded = (own_cols + 2 + 7) // 8 * 8
    width = span + 128
    out_span = span * P_SIZE // Q
    table = lanczos_table(span)
    t_high, t_low = split_table(table[reach:-reach])
    edge_high, edge_low = split_table(np.concatenate([table[:reach], table[-reach:]]))
    t_edge = np.concatenate([edge_high, edge_high, edge_low])
    t_edge = np.concatenate([t_edge[:, :128], t_edge[:, -128:]], axis=1)
    if out_span < 384:
        raise ValueError("sample count")
    vmem = pl.BlockSpec(memory_space=pltpu.VMEM)
    hbm = pl.BlockSpec(memory_space=pltpu.HBM)
    main, halo = pl.pallas_call(
        functools.partial(binning, n_xl, n_ta),
        out_shape=(pltpu.VMEM((n_pairs, own_cols, out_span), F32), pltpu.VMEM((2, reach, n_pairs * 128), F32)),
        in_specs=[hbm] * 4,
        out_specs=[vmem] * 2,
        scratch_shapes=[
            pltpu.VMEM((n_rows, n_cols, span), F32),
            pltpu.VMEM((2, n_rows, 8, span), F32),
            pltpu.VMEM((2, n_rows, n_cols), jnp.int32),
            pltpu.VMEM(t_high.shape, BF16),
            pltpu.VMEM(t_low.shape, BF16),
            pltpu.VMEM((2, n_pairs, 1, (n_cols + 32 + 127) // 128 * 128), jnp.int32),
            pltpu.VMEM((n_pairs + 2, padded, span), F32),
            pltpu.VMEM((n_pairs + 2, padded, 128), F32),
            *[pltpu.VMEM((n_pairs, 3 * height, 2 * (stop - start)), BF16)
              for start, stop, _, height in column_ranges(n_cols)],
            pltpu.VMEM((2, n_pairs + 2, 1, width), F32),
            pltpu.VMEM((2, n_pairs + 2, 1, width), F32),
            pltpu.VMEM((padded, span), F32),
            pltpu.VMEM((padded, 128), F32),
            pltpu.VMEM((2, 1, width), F32),
            pltpu.VMEM((2, reach, n_pairs * 128), F32),
            pltpu.VMEM((2, reach, n_pairs * 128), F32),
            pltpu.SemaphoreType.DMA((n_pairs,)),
            pltpu.SemaphoreType.DMA((2,)),
            pltpu.SemaphoreType.DMA((3,)),
            pltpu.SemaphoreType.DMA((8,)),
            pltpu.SemaphoreType.DMA((8,)),
        ],
        compiler_params=pltpu.CompilerParams(collective_id=0, has_side_effects=True, vmem_limit_bytes=24 * 2**20),
        name="binning",
    )(*[pltpu.with_memory_space_constraint(a, pltpu.HBM) for a in (traces, bin_steps, jnp.asarray(t_high), jnp.asarray(t_low))])
    return pl.pallas_call(
        finish,
        out_shape=jax.ShapeDtypeStruct((n_pairs, own_cols, out_span), F32),
        in_specs=[vmem] * 3,
        out_specs=hbm,
        scratch_shapes=[pltpu.VMEM((n_pairs, 2, own_cols, 128), F32), pltpu.SemaphoreType.DMA((n_pairs + 1, 2))],
        compiler_params=pltpu.CompilerParams(vmem_limit_bytes=16 * 2**20),
        name="finish",
    )(main, halo, jnp.asarray(t_edge))


def solution(mesh):
    if mesh.shape["il"] != 2:
        raise ValueError("il size")
    return jax.shard_map(
        functools.partial(shards, mesh.shape["xl"], mesh.shape["ta"]),
        mesh=mesh,
        in_specs=(P("il", "xl", "ta"), P(None, "il", "xl")),
        out_specs=P("il", "xl", "ta"),
        check_vma=False,
    )
```

```python
import functools

import numpy as np
import jax
import jax.numpy as jnp
from jax import lax
from jax.experimental import pallas as pl
from jax.experimental.pallas import tpu as pltpu
from jax.sharding import PartitionSpec as P

TAPS = 16
P_SIZE = 3
Q = 2
AHEAD = 1
MESH = pl.DeviceIdType.MESH
F32, BF16 = jnp.float32, jnp.bfloat16


def lanczos_table(span):
    reach = TAPS // 2
    rows = np.arange(span + 2 * reach)[:, None] - reach
    cols = np.arange(span * P_SIZE // Q)[None, :]
    offset = (cols * Q - rows * P_SIZE).astype(np.float64) / P_SIZE
    weights = np.sinc(offset) * np.sinc(offset / reach)
    return np.where(np.abs(offset) < reach, weights, 0.0).astype(np.float32)


def split_table(table):
    high = table.astype(BF16)
    low = (table - high.astype(np.float32)).astype(BF16)
    return high, low


def halves(values):
    high = values.astype(BF16)
    low = (values - high.astype(F32)).astype(BF16)
    return high, low


def dot(a, b):
    return jnp.dot(a, b, preferred_element_type=F32)


def column_ranges(n_cols):
    split = n_cols // 2 // 16 * 16
    if split < 16 or n_cols % 16:
        raise ValueError("column count")
    ranges = []
    for start, stop in ((0, split), (split, n_cols)):
        first = start // 2 // 8 * 8
        last = (stop - 1) // 2 + 2
        ranges.append((start, stop, first, (last + 1 - first + 7) // 8 * 8))
    return ranges


def binning(n_xl, n_ta, traces, steps_hbm, t_high_hbm, t_low_hbm, main, halo_out, x, edge_x, steps, t_high, t_low, keys,
            acc, acc_ends, one_hot_low, one_hot_high, rim_send, rim_recv, il_recv, il_recv_ends, corner_recv, halo_send, halo_recv, load_sem, edge_sem, table_sem,
            send_sem, recv_sem):
    n_rows, n_cols, span = x.shape
    n_pairs = n_rows // 2
    own_cols = n_cols // 2
    reach = TAPS // 2
    il, xl, ta = lax.axis_index("il"), lax.axis_index("xl"), lax.axis_index("ta")
    other = 1 - il
    has_xl = (xl < n_xl - 1, xl > 0)
    has_ta = (ta < n_ta - 1, ta > 0)
    xl_at, ta_at = (xl + 1, xl - 1), (ta + 1, ta - 1)

    def when(condition, work):
        pl.when(condition)(work)

    def pair(p):
        return jnp.where(il == 0, n_pairs - 1 - p, p)

    step_load = pltpu.make_async_copy(steps_hbm, steps, table_sem.at[2])
    step_load.start()
    edge_loads = [pltpu.make_async_copy(traces.at[:, pl.ds(start, 8)], edge_x.at[d], edge_sem.at[d])
                  for d, start in enumerate((n_cols - 8, 0))]
    for load in edge_loads:
        load.start()
    loads = []
    for p in range(n_pairs):
        rows = pl.ds(2 * pair(p), 2)
        loads.append(pltpu.make_async_copy(traces.at[rows], x.at[rows], load_sem.at[p]))

    barrier = pltpu.get_barrier_semaphore()

    def greet(partner):
        pl.semaphore_signal(barrier, inc=1, device_id=partner, device_id_type=MESH)

    greet({"il": other})
    for d in range(2):
        def both(d=d):
            greet({"xl": xl_at[d]})
            greet({"il": other, "xl": xl_at[d]})
        when(has_xl[d], both)
        when(has_ta[d], lambda d=d: greet({"ta": ta_at[d]}))

    def load_pair(p):
        rows = pl.ds(2 * pair(p), 2)
        pltpu.make_async_copy(traces.at[rows], x.at[rows], load_sem.at[p]).start()

    pl.loop(0, n_pairs)(load_pair)
    table_loads = [pltpu.make_async_copy(t_high_hbm, t_high, table_sem.at[0]),
                   pltpu.make_async_copy(t_low_hbm, t_low, table_sem.at[1])]
    for load in table_loads:
        load.start()

    acc[...] = jnp.zeros_like(acc)
    acc_ends[...] = jnp.zeros_like(acc_ends)
    one_hots = (one_hot_low, one_hot_high)
    step_load.wait()
    ranges = column_ranges(n_cols)
    col = lax.broadcasted_iota(jnp.int32, (n_rows, n_cols), 1)
    bin_col = lax.shift_right_logical(col, 1) + steps[1] + 1
    bin_row = steps[0] + 1
    for k, (start, stop, first, height) in enumerate(ranges):
        code = bin_row * height + bin_col - first
        for p in range(n_pairs):
            keys[k, p, :, :2 * (stop - start)] = jnp.concatenate(
                [code[2 * p: 2 * p + 1, start:stop], code[2 * p + 1: 2 * p + 2, start:stop]], axis=1)

    def one_hot(key, height):
        rows = lax.broadcasted_iota(jnp.int32, (height, key.shape[1]), 0)
        return jnp.where(rows == key, 1.0, 0.0).astype(BF16)

    def totals(chosen, values):
        high, low = halves(values)
        return (dot(chosen, high) + dot(chosen, low), dot(chosen, jnp.ones((values.shape[0], 128), BF16)))

    lane = lax.broadcasted_iota(jnp.int32, (1, 128), 1)
    is_first, is_last = lane < reach, lane >= 128 - reach

    def pair_values(at, start, stop, samples):
        return jnp.concatenate([x[2 * at, start:stop, samples], x[2 * at + 1, start:stop, samples]], axis=0)

    def bin_edges(p):
        at = pair(p)
        loads[p].wait()
        for k, (start, stop, first, height) in enumerate(ranges):
            chosen = one_hot(keys[k, at][:, :2 * (stop - start)], 3 * height)
            one_hots[k][at] = chosen
            values = jnp.where(lane < 64, pair_values(at, start, stop, slice(0, 128)),
                               pair_values(at, start, stop, slice(span - 128, span)))
            high = values.astype(BF16)
            low = jnp.where(is_first | is_last, values - high.astype(F32), 1.0).astype(BF16)
            sums = dot(chosen, jnp.concatenate([high, low], axis=1))
            ends = jnp.where(is_first | is_last, sums[:, :128], 0.0) + sums[:, 128:]
            for r in range(3):
                acc_ends[at + r, first: first + height, :] += ends[r * height: (r + 1) * height]

    def bin_pair(p):
        at = pair(p)
        for k, (start, stop, first, height) in enumerate(ranges):
            chosen = one_hots[k][at]
            high, low = halves(pair_values(at, start, stop, slice(0, span)))
            sums = dot(chosen, high) + dot(chosen, low)
            for r in range(3):
                acc[at + r, first: first + height, :] += sums[r * height: (r + 1) * height]

    def remote(src, dst, slot, partner):
        return pltpu.make_async_remote_copy(src_ref=src, dst_ref=dst, send_sem=send_sem.at[slot],
                                            recv_sem=recv_sem.at[slot], device_id=partner, device_id_type=MESH)

    rim_row = jnp.where(il == 0, n_pairs + 1, 0)
    own_row = jnp.where(il == 0, n_pairs, 1)
    to_other = remote(acc.at[rim_row], il_recv, 0, {"il": other})
    ends_to_other = remote(acc_ends.at[rim_row], il_recv_ends, 7, {"il": other})
    rims = [(remote(rim_send.at[d], rim_recv.at[d], 1 + d, {"xl": xl_at[d]}),
             remote(rim_send.at[d, rim_row], corner_recv.at[d], 3 + d, {"il": other, "xl": xl_at[d]}))
            for d in range(2)]

    row = lax.broadcasted_iota(jnp.int32, (n_rows, n_cols), 0)
    rim_bin = bin_row + lax.shift_right_logical(row, 1)
    for load in edge_loads:
        load.wait()
    for d, (start, column) in enumerate(((n_cols - 8, own_cols + 1), (0, 0))):
        target = jnp.where(bin_col == column, rim_bin, -1)
        key = jnp.concatenate([target[i: i + 1, start: start + 8] for i in range(n_rows)], axis=1)
        sums, folds = totals(one_hot(key, (n_pairs + 2 + 7) // 8 * 8), edge_x[d].reshape(n_rows * 8, span))
        for r in range(n_pairs + 2):
            rim_send[d, r, :, :span] = sums[r: r + 1]
            rim_send[d, r, :, span:] = jnp.where(is_first, sums[r: r + 1, :128], jnp.where(
                is_last, sums[r: r + 1, span - 128:], folds[r: r + 1]))
    peers = 1
    for d in range(2):
        peers = peers + jnp.where(has_xl[d], 2, 0) + jnp.where(has_ta[d], 1, 0)
    pl.semaphore_wait(barrier, peers)
    for d in range(2):
        def go(d=d):
            for copy in rims[d]:
                copy.start()
        when(has_xl[d], go)
    bin_edges(0)
    ends_to_other.start()
    for p in range(1, n_pairs):
        bin_edges(p)
    for p in range(AHEAD):
        bin_pair(p)
        if p == 0:
            to_other.start()
    ends_to_other.wait_recv()
    acc_ends[own_row] = acc_ends[own_row] + il_recv_ends[...]
    for d, column in enumerate((1, own_cols)):
        def add_ends(d=d, column=column):
            for copy in rims[d]:
                copy.wait_recv()
            for r in range(1, n_pairs + 1):
                acc_ends[r, column: column + 1, :] += rim_recv[d, r, :, span:]
            acc_ends[own_row, column: column + 1, :] += corner_recv[d, :, span:]
        when(has_xl[1 - d], add_ends)

    halos = [remote(halo_send.at[d], halo_recv.at[d], 5 + d, {"ta": ta_at[d]}) for d in range(2)]
    for b in range(n_pairs):
        lanes = slice(b * 128, b * 128 + own_cols)
        ends = acc_ends[b + 1, 1: own_cols + 1, :].T
        factor = 1.0 / jnp.maximum(ends[64:64 + reach], 1.0)
        halo_send[0, :, lanes] = ends[128 - reach:] * factor
        halo_send[1, :, lanes] = ends[:reach] * factor
    for d in range(2):
        when(has_ta[d], halos[d].start)

    for p in range(AHEAD, n_pairs):
        bin_pair(p)
        if p == 0:
            to_other.start()
    to_other.wait_recv()
    acc[own_row] = acc[own_row] + il_recv[...]
    for d, column in enumerate((1, own_cols)):
        def add(d=d, column=column):
            for r in range(1, n_pairs + 1):
                acc[r, column: column + 1, :] += rim_recv[d, r, :, :span]
            acc[own_row, column: column + 1, :] += corner_recv[d, :, :span]
        when(has_xl[1 - d], add)
    for load in table_loads:
        load.wait()
    for b in range(n_pairs):
        fold = jnp.broadcast_to(acc_ends[b + 1, 1: own_cols + 1, 64:65], (own_cols, 128))
        factor = 1.0 / jnp.maximum(fold, 1.0)
        sums = acc[b + 1, 1: own_cols + 1, :]
        high, low = halves(sums * jnp.concatenate([factor] * (span // 128), axis=1))
        main[b] = dot(high, t_high[...]) + (dot(low, t_high[...]) + dot(high, t_low[...]))
    for d in range(2):
        def arrived(d=d):
            halos[d].wait_recv()
            halo_out[d] = halo_recv[d]

        def absent(d=d):
            halo_out[d] = jnp.zeros_like(halo_recv[d])
        when(has_ta[1 - d], arrived)
        when(jnp.logical_not(has_ta[1 - d]), absent)
    for d in range(2):
        when(has_ta[d], halos[d].wait_send)
        def sent(d=d):
            for copy in rims[d]:
                copy.wait_send()
        when(has_xl[d], sent)
    to_other.wait_send()
    ends_to_other.wait_send()


def finish(main, halo, t_edge, out, staged, out_sem):
    n_pairs, own_cols, width = main.shape
    inner = pl.ds(128, width - 256)
    writes = [pltpu.make_async_copy(main.at[:, :, inner], out.at[:, :, inner], out_sem.at[n_pairs, 0])]
    writes[0].start()
    for b in range(n_pairs):
        lanes = slice(b * 128, (b + 1) * 128)
        edges = jnp.concatenate([halo[0, :, lanes], halo[1, :, lanes]], axis=0)
        high = edges.astype(BF16).astype(F32)
        terms = jnp.concatenate([high, edges - high, high], axis=0).T[:own_cols].astype(BF16)
        ends = dot(terms, t_edge[...])
        for d, start in enumerate((0, width - 128)):
            staged[b, d] = main[b, :, start: start + 128] + ends[:, d * 128: (d + 1) * 128]
            write = pltpu.make_async_copy(staged.at[b, d], out.at[b, :, pl.ds(start, 128)], out_sem.at[b, d])
            write.start()
            writes.append(write)
    for write in writes:
        write.wait()


def shards(n_xl, n_ta, traces, bin_steps):
    n_rows, n_cols, span = traces.shape
    n_pairs, own_cols = n_rows // 2, n_cols // 2
    reach = TAPS // 2
    padded = (own_cols + 2 + 7) // 8 * 8
    width = span + 128
    out_span = span * P_SIZE // Q
    table = lanczos_table(span)
    t_high, t_low = split_table(table[reach:-reach])
    edge_high, edge_low = split_table(np.concatenate([table[:reach], table[-reach:]]))
    t_edge = np.concatenate([edge_high, edge_high, edge_low])
    t_edge = np.concatenate([t_edge[:, :128], t_edge[:, -128:]], axis=1)
    if out_span < 384:
        raise ValueError("sample count")
    vmem = pl.BlockSpec(memory_space=pltpu.VMEM)
    hbm = pl.BlockSpec(memory_space=pltpu.HBM)
    main, halo = pl.pallas_call(
        functools.partial(binning, n_xl, n_ta),
        out_shape=(pltpu.VMEM((n_pairs, own_cols, out_span), F32), pltpu.VMEM((2, reach, n_pairs * 128), F32)),
        in_specs=[hbm] * 4,
        out_specs=[vmem] * 2,
        scratch_shapes=[
            pltpu.VMEM((n_rows, n_cols, span), F32),
            pltpu.VMEM((2, n_rows, 8, span), F32),
            pltpu.VMEM((2, n_rows, n_cols), jnp.int32),
            pltpu.VMEM(t_high.shape, BF16),
            pltpu.VMEM(t_low.shape, BF16),
            pltpu.VMEM((2, n_pairs, 1, (n_cols + 32 + 127) // 128 * 128), jnp.int32),
            pltpu.VMEM((n_pairs + 2, padded, span), F32),
            pltpu.VMEM((n_pairs + 2, padded, 128), F32),
            *[pltpu.VMEM((n_pairs, 3 * height, 2 * (stop - start)), BF16)
              for start, stop, _, height in column_ranges(n_cols)],
            pltpu.VMEM((2, n_pairs + 2, 1, width), F32),
            pltpu.VMEM((2, n_pairs + 2, 1, width), F32),
            pltpu.VMEM((padded, span), F32),
            pltpu.VMEM((padded, 128), F32),
            pltpu.VMEM((2, 1, width), F32),
            pltpu.VMEM((2, reach, n_pairs * 128), F32),
            pltpu.VMEM((2, reach, n_pairs * 128), F32),
            pltpu.SemaphoreType.DMA((n_pairs,)),
            pltpu.SemaphoreType.DMA((2,)),
            pltpu.SemaphoreType.DMA((3,)),
            pltpu.SemaphoreType.DMA((8,)),
            pltpu.SemaphoreType.DMA((8,)),
        ],
        compiler_params=pltpu.CompilerParams(collective_id=0, has_side_effects=True, vmem_limit_bytes=24 * 2**20),
        name="binning",
    )(*[pltpu.with_memory_space_constraint(a, pltpu.HBM) for a in (traces, bin_steps, jnp.asarray(t_high), jnp.asarray(t_low))])
    return pl.pallas_call(
        finish,
        out_shape=jax.ShapeDtypeStruct((n_pairs, own_cols, out_span), F32),
        in_specs=[vmem] * 3,
        out_specs=hbm,
        scratch_shapes=[pltpu.VMEM((n_pairs, 2, own_cols, 128), F32), pltpu.SemaphoreType.DMA((n_pairs + 1, 2))],
        compiler_params=pltpu.CompilerParams(vmem_limit_bytes=16 * 2**20),
        name="finish",
    )(main, halo, jnp.asarray(t_edge))


def solution(mesh):
    if mesh.shape["il"] != 2:
        raise ValueError("il size")
    return jax.shard_map(
        functools.partial(shards, mesh.shape["xl"], mesh.shape["ta"]),
        mesh=mesh,
        in_specs=(P("il", "xl", "ta"), P(None, "il", "xl")),
        out_specs=P("il", "xl", "ta"),
        check_vma=False,
    )
```
